32 devices in a mesh: freq: 8 (over z, x), sens: 4 (over y, core).
Axes of the slice: x: 2, y: 2, z: 4, core: 2. Of those that a mesh axis runs over, the one named last changes fastest.
Arguments:
- samples: bfloat16 [128, 608, 420], P('freq', 'sens'), may hold values from -6 to 6
- response_tiles: bfloat16 [448, 2, 608, 21], P('freq', None, 'sens'), may hold values from -0.25 to 0.25
- slot_sensor: int32 [608], P('sens'), may hold values from -1 to 599, as said below
- sensor_noise: float32 [600], replicated, may hold values from 0.02 to 5
- advance_offset: int32 [21], replicated, may hold values from 0 to 419
Outputs:
- outlook_values: bfloat16 [128, 21, 420], P('freq')
- noise_spread: float32 [21], replicated
The draws below stay inside these ranges and needn't reach their ends.
Inputs may be any that keep to these rules, and one draw needn't show every extreme that they name: `slot_sensor`: every sensor number appears in exactly one slot; the other 8 slots hold -1.
All inputs are finite; a program needn't handle non-finite values.
Results may differ from the reference program's by a relative error of at most 0.0055.
Values may be sent and summed in bfloat16 or wider, within the bound.
A program may use at most 64 MiB of HBM per device.

```python
import math
import jax
import jax.numpy as jnp
from jax import lax

TARGET_PLACES = 21
PROBE_COUNT = 600
HORIZON_LENGTH = 420
KEPT_HARMONICS = 448
POSTERIOR_COUNT = 128
PROBE_POSITIONS = 608
N_FREQ = 8


def draw_slot_sensor(key, part):
    ordering = jax.random.permutation(key, PROBE_POSITIONS).astype(jnp.int32)
    return jnp.where(ordering < PROBE_COUNT, ordering, -1).astype(jnp.int32)


def place_ends(drawn, rng, least, largest):
    spot = [jax.random.randint(jax.random.fold_in(rng, axis), (), 0, length) for axis, length in enumerate(drawn.shape)]
    main_axis = drawn.shape.index(max(drawn.shape))
    beside = spot[:main_axis] + [(spot[main_axis] + 1) % drawn.shape[main_axis]] + spot[main_axis + 1:]
    return drawn.at[tuple(spot)].set(least).at[tuple(beside)].set(largest)


def block_scale(own_key, dims, pieces, low, high):
    def one(position, blocks):
        draws = jax.random.uniform(jax.random.fold_in(jax.random.fold_in(own_key, 6), position), (blocks,), jnp.float32, low / len(pieces), high / len(pieces))
        return jnp.repeat(jnp.exp(draws), dims[position] // blocks).reshape((-1,) + (1,) * (len(dims) - position - 1))

    level = one(*pieces[0])
    for cut in pieces[1:]:
        level = level * one(*cut)
    return level


def noise(own_key, shape, spread, bound, shards=(), held_as=jnp.bfloat16):
    gain = block_scale(own_key, shape, shards, -0.22, 0.18) if shards else 1.0
    array = jax.random.normal(own_key, shape, jnp.float32) * spread * gain
    return jnp.minimum(jnp.maximum(array, -bound), bound).astype(held_as)


def setup_inputs(seed: int = 0) -> dict:
    splits = jax.random.split(jax.random.key(seed), 6)
    return {
        "samples": noise(splits[0], (POSTERIOR_COUNT, PROBE_POSITIONS, HORIZON_LENGTH), 1.0, 6.0, ((0, 8), (1, 4))),
        "response_tiles": noise(splits[1], (KEPT_HARMONICS, 2, PROBE_POSITIONS, TARGET_PLACES), (PROBE_COUNT * HORIZON_LENGTH // KEPT_HARMONICS) ** -0.5, 0.25, ((0, 8), (2, 4))),
        "slot_sensor": draw_slot_sensor(jax.random.fold_in(splits[5], 71), 0),
        "sensor_noise": jnp.clip(jnp.exp(jax.random.uniform(splits[3], (PROBE_COUNT,), jnp.float32, math.log(0.02), math.log(5.0))), 0.02, 5.0),
        "advance_offset": place_ends(jax.random.randint(splits[4], (TARGET_PLACES,), 0, HORIZON_LENGTH), jax.random.fold_in(splits[4], 1), 0, HORIZON_LENGTH - 1).astype(jnp.int32),
    }


def angles(first_bin, bin_count, period, factor):
    bin_index = first_bin + lax.iota(jnp.int32, bin_count)
    turn_count = (bin_index[:, None] * factor[None, :]) % period
    return turn_count.astype(jnp.float32) * (2.0 * math.pi / period)


def forward_table(bin_count, step_count, period):
    phase_angle = angles(0, bin_count, period, lax.iota(jnp.int32, step_count))
    return jnp.stack([jnp.cos(phase_angle), -jnp.sin(phase_angle)]).astype(jnp.bfloat16)


def inverse_table(bin_count, step_count, period):
    bin_index = lax.iota(jnp.int32, bin_count)
    weight = jnp.where(bin_index == 0, 1.0, 2.0).astype(jnp.float32) / period
    phase_angle = angles(0, bin_count, period, lax.iota(jnp.int32, step_count))
    return jnp.stack([weight[:, None] * jnp.cos(phase_angle), -weight[:, None] * jnp.sin(phase_angle)])


def reference(samples, response_tiles, slot_sensor, sensor_noise, advance_offset):
    period = 2 * KEPT_HARMONICS
    highest = lax.Precision.HIGHEST
    live_slot = (slot_sensor >= 0).astype(jnp.bfloat16)
    blocks = response_tiles * live_slot[None, None, :, None]
    wide = blocks.astype(jnp.float32)
    sensor_ids = lax.iota(jnp.int32, PROBE_COUNT)
    slot_noise = jnp.sum(jnp.where(slot_sensor[:, None] == sensor_ids[None, :], sensor_noise[None, :], jnp.float32(0.0)), axis=1)
    power = wide[:, 0] * wide[:, 0] + wide[:, 1] * wide[:, 1]
    bin_index = lax.iota(jnp.int32, KEPT_HARMONICS)
    bin_weight = jnp.where(bin_index == 0, 1.0, 2.0).astype(jnp.float32) / period
    per_bin = jnp.einsum("ksq,s->kq", power, slot_noise, precision=highest)
    noise_spread = jnp.dot(bin_weight, per_bin, precision=highest)

    forward_flat = forward_table(KEPT_HARMONICS, HORIZON_LENGTH, period).reshape(2 * KEPT_HARMONICS, HORIZON_LENGTH)
    backward = inverse_table(KEPT_HARMONICS, HORIZON_LENGTH, period).astype(jnp.float32)
    block_real = wide[:, 0]
    block_imag = wide[:, 1]
    twiddle = angles(0, KEPT_HARMONICS, period, advance_offset)
    cosine = jnp.cos(twiddle)[:, :, None]
    sine_part = jnp.sin(twiddle)[:, :, None]

    def product(left, right):
        return jnp.einsum("krs,ksq->kqr", left, right, precision=highest)

    def single_block(sample_block):
        row_count = sample_block.shape[0]
        flat_out = jnp.dot(sample_block.reshape(row_count * PROBE_POSITIONS, HORIZON_LENGTH), forward_flat.T, preferred_element_type=jnp.float32)
        spectra = flat_out.reshape(row_count, PROBE_POSITIONS, 2, KEPT_HARMONICS).transpose(2, 3, 0, 1).astype(jnp.bfloat16)
        spec_real = spectra[0].astype(jnp.float32)
        spec_imag = spectra[1].astype(jnp.float32)
        real_part = product(spec_real, block_real) - product(spec_imag, block_imag)
        imag_part = product(spec_real, block_imag) + product(spec_imag, block_real)
        shifted = jnp.stack([real_part * cosine - imag_part * sine_part, real_part * sine_part + imag_part * cosine])
        return jnp.einsum("ckqr,ckt->rqt", shifted, backward, precision=highest).astype(jnp.bfloat16)

    estimate_tiles = lax.map(single_block, samples.reshape(N_FREQ, POSTERIOR_COUNT // N_FREQ, PROBE_POSITIONS, HORIZON_LENGTH))
    outlook_values = estimate_tiles.reshape(POSTERIOR_COUNT, TARGET_PLACES, HORIZON_LENGTH)
    return (outlook_values, noise_spread)
```

```python
import functools
import math

import jax
import jax.numpy as jnp
import numpy as np
from jax import lax
from jax.experimental import pallas as pl
from jax.experimental.pallas import tpu as pltpu
from jax.sharding import PartitionSpec as P

MESH = pl.DeviceIdType.MESH
HALF = 64
LANES = 128
SEAT = 32


class Plan:
    def __init__(self, bins_dev, slots, sites, halves):
        self.bins_dev, self.slots, self.sites = bins_dev, slots, sites
        self.group = HALF // sites
        self.chunks = -(-bins_dev // self.group)
        full = self.chunks // 2
        cut = -(-slots // 32) * 16
        plus = [(c, 0, slots) for c in range(full)]
        minus = [(c, 0, slots) for c in range(self.chunks - full, self.chunks)]
        if self.chunks % 2:
            plus.append((full, 0, cut))
            minus.append((full, cut, slots))
        self.parts = (plus, minus)
        self.m = len(plus)
        self.pad = -(-self.m // 16) * 16
        self.rows = [sum(hi - lo for _, lo, hi in part) for part in self.parts]
        self.held_rows = -(-max(self.rows) // 16) * 16
        ends = [-(-self.m * h // halves) for h in range(halves + 1)]
        self.halves = halves
        self.spans = list(zip(ends[:-1], ends[1:]))
        self.pieces = [(d, h) for h in range(halves) for d in range(2)]

    def size(self, chunk):
        return min(self.group, self.bins_dev - chunk * self.group)

    def row(self, d, k):
        return sum(hi - lo for _, lo, hi in self.parts[d][:k])


def make_tables(freq_size, plan, step_count):
    bins_dev, group, chunks = plan.bins_dev, plan.group, plan.chunks
    period = 2 * freq_size * bins_dev
    slot = np.arange(freq_size * chunks * group)
    block, inside = slot // (chunks * group), slot % (chunks * group)
    live = (inside < bins_dev).astype(np.float64)
    bins = np.where(inside < bins_dev, block * bins_dev + inside, 0)
    turns = bins[:, None] * np.arange(step_count)[None, :] % period
    angle = turns * (2.0 * math.pi / period)
    forward = np.stack([np.cos(angle), -np.sin(angle)]) * live[None, :, None]
    inverse = np.zeros((freq_size, 2, group, 2, plan.pad, step_count))
    weight = (np.where(bins == 0, 1.0, 2.0) / period).reshape(freq_size, chunks, group)
    table = forward.reshape(2, freq_size, chunks, group, step_count) * weight[None, ..., None]
    for d in range(2):
        for k, (chunk, _, _) in enumerate(plan.parts[d]):
            inverse[:, :, :, d, k] = table[:, :, chunk].transpose(1, 0, 2, 3)
    return forward, inverse.reshape(freq_size, 4 * group * plan.pad, step_count)


def kernel(
    freq_size, sens_size, plan,
    tiles_in, samples_in, forward_in, inverse_in, slots_in, noise_in, offsets_in,
    out, spread_out,
    raw, samples, forward, inverse, ids, noise, offsets, load_sem, tile_sem,
    facts, live, cosine, sine, weight,
    held, spectra, z_own, z_send, z_recv, turned_z, gathered, total, spread, spread_send, spread_recv,
    ring_send, ring_recv, z_send_sem, z_recv_sem, s_send_sem, s_recv_sem,
):
    rows, slots, step_count = samples.shape
    n, group, chunks, sites, m, pad = freq_size, plan.group, plan.chunks, plan.sites, plan.m, plan.pad
    bins_dev = plan.bins_dev
    per_bin = 2 * rows
    lane_tiles = spectra.shape[0]
    period = 2 * n * bins_dev
    pieces, halves = plan.pieces, plan.halves
    me_f = lax.axis_index("freq")
    me_s = lax.axis_index("sens")

    def position_of(index):
        odd, pair = lax.rem(index, 2), index // 2
        return pair * (1 - odd) + (n - 1 - pair) * odd

    def index_of(position):
        high = position // (n // 2)
        return 2 * position * (1 - high) + (2 * (n - 1 - position) + 1) * high

    me_p = position_of(me_f)

    def along(step):
        return index_of(lax.rem(me_p + step + 2 * n, n))

    def origin_of(d, arrival):
        return along(arrival if d else -arrival)

    right, left = along(1), along(-1)
    barrier = pltpu.get_barrier_semaphore()
    for neighbour in (left, right):
        pl.semaphore_signal(barrier, inc=1, device_id={"freq": neighbour}, device_id_type=MESH)
    for d in range(1, sens_size):
        peer = lax.rem(me_s + d, sens_size)
        pl.semaphore_signal(barrier, inc=1, device_id={"sens": peer}, device_id_type=MESH)

    tile_loads = []
    for at, (d, h) in enumerate(pieces):
        needed = [
            chunk for chunk, low, high in plan.parts[d][slice(*plan.spans[h])]
            if d == 0 or high - low == slots
        ]
        if needed:
            low = needed[0] * group
            span = pl.ds(low, min((needed[-1] + 1) * group, bins_dev) - low)
            tile_loads.append([pltpu.make_async_copy(tiles_in.at[span], raw.at[span], tile_sem.at[at])])
        else:
            tile_loads.append([])
    loads = [
        pltpu.make_async_copy(source, target, load_sem.at[at])
        for at, (source, target) in enumerate((
            (slots_in, ids), (noise_in, noise), (offsets_in, offsets),
            (forward_in, forward), (samples_in, samples), (inverse_in, inverse),
        ))
    ]
    for load in sum(tile_loads, []) + loads:
        load.start()

    def ring_copy(step, piece, received):
        d, h = piece
        low, high = (plan.row(d, k) for k in plan.spans[h])
        origin = origin_of(d, step + (1 if received else 0))
        block = held.at[d, origin, pl.ds(low, high - low)]
        at = 2 * h + d
        return pltpu.make_async_remote_copy(
            src_ref=block, dst_ref=block,
            send_sem=ring_send.at[at, step], recv_sem=ring_recv.at[at, step],
            device_id={"freq": left if d else right}, device_id_type=MESH,
        )

    line = lax.broadcasted_iota(jnp.int32, (group * sites * 2, LANES), 0)
    spot = lax.broadcasted_iota(jnp.int32, (group * sites * 2, LANES), 1)
    sorter = (spot == lax.rem(line, 2) * HALF + line // 2).astype(jnp.float32).astype(jnp.bfloat16)

    def sort_tiles(d, h):
        for k in range(*plan.spans[h]):
            chunk, low, high = plan.parts[d][k]
            whole = (low, high) == (0, slots)
            if d and not whole:
                continue
            size = plan.size(chunk)
            block = raw[chunk * group:chunk * group + size].reshape(size * sites * 2, slots)
            turned = lax.dot_general(
                block, sorter[:size * sites * 2], (((0,), (0,)), ((), ())),
                preferred_element_type=jnp.float32,
            ).astype(jnp.bfloat16)
            at = plan.row(d, k)
            held[d, me_f, at:at + high - low] = turned[low:high]
            if not whole:
                at = plan.row(1, m - 1)
                held[1, me_f, at:at + slots - high] = turned[high:]

    for at, piece in enumerate(pieces):
        for load in tile_loads[at]:
            load.wait()
        sort_tiles(*piece)
        if at == 0:
            pl.semaphore_wait(barrier, 2 + sens_size - 1)
        ring_copy(0, piece, False).start()

    for load in loads[:3]:
        load.wait()

    def fact(s, carry):
        sensor = ids[s]
        there = (sensor >= 0).astype(jnp.float32)
        facts[0, pl.ds(s, 1), :] = jnp.full((1, LANES), noise[jnp.maximum(sensor, 0)] * there)
        facts[1, pl.ds(s, 1), :] = jnp.full((1, LANES), there)
        return carry

    lax.fori_loop(0, slots, fact, 0, unroll=8)
    there = facts[1].astype(jnp.bfloat16)
    live[...] = jnp.concatenate([there] * (live.shape[1] // LANES), axis=1)
    spread[...] = jnp.zeros_like(spread)
    turned_z[...] = jnp.zeros_like(turned_z)
    total[...] = jnp.zeros_like(total)

    lane = lax.broadcasted_iota(jnp.int32, (rows, LANES), 1)
    which = (lane % HALF) // sites
    sign = jnp.where(lane < HALF, -1.0, 1.0).astype(jnp.float32)

    place = lax.broadcasted_iota(jnp.int32, (2 * pad, LANES), 1)
    seat = lax.broadcasted_iota(jnp.int32, (2 * pad, LANES), 0)
    inside = place % HALF
    lead = jnp.zeros((2 * pad, LANES), jnp.float32)
    for q in range(sites):
        lead = jnp.where(inside % sites == q, offsets[q].astype(jnp.float32), lead)
    side = seat // pad
    chunk_of = jnp.zeros_like(seat)
    for d in range(2):
        for k in range(m):
            chunk_of = jnp.where(seat == d * pad + k, plan.parts[d][k][0], chunk_of)
    within = chunk_of * group + inside // sites
    alive = (within < bins_dev) & (inside < group * sites) & (seat % pad < m)
    turning = 2.0 * math.pi / period

    def phase(arrival, carry):
        block = jnp.where(side == 0, origin_of(0, arrival), origin_of(1, arrival))
        bins = block * bins_dev + within
        ahead = bins.astype(jnp.float32) * lead
        angle = (ahead - period * jnp.floor(ahead / period)) * turning
        here = pl.ds(pl.multiple_of(arrival * 2 * pad, 2 * pad), 2 * pad)
        cosine[here, :] = jnp.cos(angle)
        sine[here, :] = jnp.sin(angle) * jnp.where(place < HALF, -1.0, 1.0)
        weight[here, :] = jnp.where(alive, jnp.where(bins == 0, 1.0, 2.0) / period, 0.0)
        return carry

    lax.fori_loop(0, n, phase, 0)

    def transform(r):
        sample = samples[r] * live[:, :step_count]
        for c in range(2):
            value = lax.dot_general(
                forward[c], sample, (((1,), (1,)), ((), ())),
                preferred_element_type=jnp.float32,
            )
            for tile in range(lane_tiles):
                part = value[:, tile * LANES:min(slots, (tile + 1) * LANES)]
                if part.shape[1] < LANES:
                    part = jnp.concatenate(
                        [part, jnp.zeros((part.shape[0], LANES - part.shape[1]), part.dtype)], axis=1
                    )
                spectra[tile, pl.ds(c * rows + r, part.shape[0], stride=per_bin), :] = part

    def transforms(low, high):
        lax.fori_loop(low, high, lambda r, carry: (transform(r), carry)[1], 0)

    def z_row(arrival, d, k):
        return (arrival * 2 + d) * m + k

    def contract(arrival, piece):
        d, h = piece
        origin = origin_of(d, arrival)
        noisy = spread[...]
        for k in range(*plan.spans[h]):
            chunk, low, high = plan.parts[d][k]
            row = plan.row(d, k)
            weights = held[d, origin, row:row + high - low]
            first = pl.multiple_of((origin * chunks + chunk) * (group * per_bin), group * per_bin)
            parts = [spectra[tile, pl.ds(first, group * per_bin), :] for tile in range(lane_tiles)]
            spec = jnp.concatenate(parts, axis=1)[:, :slots].astype(jnp.bfloat16)
            filled = weights
            if high - low < slots:
                filled = jnp.concatenate(
                    ([jnp.zeros((low, LANES), jnp.bfloat16)] if low else []) + [weights]
                    + ([jnp.zeros((slots - high, LANES), jnp.bfloat16)] if high < slots else []), axis=0
                )
            product = jnp.dot(spec, filled, preferred_element_type=jnp.float32)
            picked = [product[c * rows:(c + 1) * rows] for c in range(2)]
            for i in range(1, group):
                for c in range(2):
                    at = i * per_bin + c * rows
                    picked[c] = jnp.where(which == i, product[at:at + rows], picked[c])
            value = picked[0] + sign * pltpu.roll(picked[1], HALF, 1)
            at = z_row(arrival, d, k)
            z_own[pl.ds(pl.multiple_of(at * rows, rows), rows), :] = value
            z_send[at] = value.astype(jnp.bfloat16)
            wide = weights.astype(jnp.float32)
            power = wide * wide * facts[0, low:high]
            power = power.reshape((high - low) // 8, 8, LANES).sum(axis=0)
            noisy += power * weight[pl.ds(arrival * 2 * pad + d * pad + k, 1), :]
        spread[...] = noisy

    def z_copies(arrival, piece):
        d, h = piece
        low, high = plan.spans[h]
        part = pl.ds(z_row(arrival, d, low), high - low)
        at = arrival * len(pieces) + 2 * h + d
        return [
            pltpu.make_async_remote_copy(
                src_ref=z_send.at[part], dst_ref=z_recv.at[p - 1, part],
                send_sem=z_send_sem.at[p - 1, at], recv_sem=z_recv_sem.at[p - 1, at],
                device_id={"sens": lax.rem(me_s + p, sens_size)}, device_id_type=MESH,
            )
            for p in range(1, sens_size)
        ]

    def send_z(arrival, piece):
        for copy in z_copies(arrival, piece):
            copy.start()

    def receive(step, piece, last=False):
        ring_copy(step, piece, True).wait_recv()
        if not last:
            ring_copy(step + 1, piece, False).start()

    together = LANES // SEAT
    seat_of = lax.broadcasted_iota(jnp.int32, (pad, LANES), 1) // SEAT

    def finish(arrival):
        for piece in pieces:
            for copy in z_copies(arrival, piece):
                copy.wait_recv()
        for d in range(2):
            for k in range(m):
                at = z_row(arrival, d, k)
                value = z_own[pl.ds(pl.multiple_of(at * rows, rows), rows), :]
                for p in range(1, sens_size):
                    value += z_recv[p - 1, at].astype(jnp.float32)
                near = pl.ds(arrival * 2 * pad + d * pad + k, 1)
                turned_z[d, k * rows:(k + 1) * rows] = (
                    value * cosine[near, :] + pltpu.roll(value, HALF, 1) * sine[near, :]
                )
        for d in range(2):
            for base in range(0, rows, together):
                mine = [turned_z[d, pl.ds(base + j, pad, stride=rows), :] for j in range(together)]
                for c in range(2):
                    for i in range(group):
                        start = c * HALF + i * sites
                        value = None
                        for j in range(together):
                            moved = pltpu.roll(mine[j], (j * SEAT - start) % LANES, 1)
                            value = moved if value is None else jnp.where(seat_of == j, moved, value)
                        low = ((c * group + i) * 2 + d) * pad
                        gathered[low:low + pad, base * SEAT:(base + together) * SEAT] = value.astype(jnp.bfloat16)
        origins = [origin_of(d, arrival) for d in range(2)]
        table = jnp.concatenate(
            [
                inverse[origins[d], at * pad:(at + 1) * pad]
                for at, d in ((2 * ci + d, d) for ci in range(2 * group) for d in range(2))
            ], axis=0
        )
        return lax.dot_general(
            gathered[...], table, (((0,), (0,)), ((), ())), preferred_element_type=jnp.float32
        )

    def finished(low, high):
        def one(arrival, carry):
            total[...] += finish(arrival)
            return carry

        lax.fori_loop(low, high, one, 0)

    for load in loads[3:5]:
        load.wait()
    turns = 3 * halves - (1 if halves > 1 else 0)
    shares = [0] + [rows // 8 + (rows - rows // 8) * turn // turns for turn in range(turns + 1)]
    transforms(shares[0], shares[1])
    for step in range(3):
        for h in range(halves):
            for d in range(2):
                receive(step, (d, h))
            at = halves * step + h + 1
            if at + 1 < len(shares):
                transforms(shares[at], shares[at + 1])
    loads[5].wait()

    def contracts(low, high, piece):
        lax.fori_loop(low, high, lambda arrival, carry: (contract(arrival, piece), carry)[1], 0)

    def both(step, carry):
        low = 2 * (step - 3)
        for h in range(halves):
            for d in range(2):
                receive(step, (d, h))
            for d in range(2):
                contracts(low, low + 2, (d, h))
            for arrival in (low, low + 1):
                for d in range(2):
                    send_z(arrival, (d, h))
            if h == 0:
                finished(jnp.maximum(low - 2, 0), low)
        return carry

    lax.fori_loop(3, 6, both, 0)

    def single(step, carry):
        for h in range(halves):
            for d in range(2):
                receive(step, (d, h))
            for d in range(2):
                contract(step, (d, h))
                send_z(step, (d, h))
            if h == 0:
                finished(step - 2, step - 1)
        return carry

    if n > 8:
        lax.fori_loop(6, n - 2, single, 0)
    for piece in pieces:
        contracts(n - 2, n - 1, piece)
        send_z(n - 2, piece)
    finished(n - 4, n - 2)
    for h in range(halves):
        for d in range(2):
            receive(n - 2, (d, h), True)
            contract(n - 1, (d, h))
            send_z(n - 1, (d, h))
        if h == 0:
            finished(n - 2, n - 1)
    spread_send[...] = spread[...]
    spread_copies = [
        pltpu.make_async_remote_copy(
            src_ref=spread_send, dst_ref=spread_recv.at[p - 1],
            send_sem=s_send_sem.at[p - 1], recv_sem=s_recv_sem.at[p - 1],
            device_id={"sens": lax.rem(me_s + p, sens_size)}, device_id_type=MESH,
        )
        for p in range(1, sens_size)
    ]
    for copy in spread_copies:
        copy.start()
    for step in range(n - 1):
        for piece in pieces:
            ring_copy(step, piece, False).wait_send()
    for arrival in range(n - 1):
        for piece in pieces:
            for copy in z_copies(arrival, piece):
                copy.wait_send()
    result = total[...] + finish(n - 1)
    for r in range(rows):
        out[r] = result[r * SEAT:r * SEAT + sites].astype(jnp.bfloat16)
    for copy in spread_copies:
        copy.wait()
    summed = spread[...]
    for p in range(1, sens_size):
        summed += spread_recv[p - 1]
    summed = jnp.broadcast_to(jnp.sum(summed, axis=0, keepdims=True), summed.shape)
    summed = summed + pltpu.roll(summed, HALF, 1)
    folded = summed
    for i in range(1, group):
        folded += pltpu.roll(summed, LANES - i * sites, 1)
    spread_out[...] = folded
    for piece in pieces:
        for copy in z_copies(n - 1, piece):
            copy.wait_send()


def on_device(freq_size, sens_size, samples, response_tiles, slot_sensor, sensor_noise, advance_offset):
    bins_dev, _, slots, sites = response_tiles.shape
    rows, _, step_count = samples.shape
    peers = sens_size - 1
    plan = Plan(bins_dev, slots, sites, 2 if peers * freq_size * 4 <= 1024 else 1)
    group, chunks, m, pad = plan.group, plan.chunks, plan.m, plan.pad
    forward, inverse = make_tables(freq_size, plan, step_count)
    tiles = response_tiles.transpose(0, 3, 1, 2)
    lane_tiles = -(-slots // LANES)
    count = len(plan.pieces)
    wide = -(-step_count // LANES) * LANES
    vmem = pl.BlockSpec(memory_space=pltpu.VMEM)
    anywhere = pl.BlockSpec(memory_space=pl.ANY)
    outlook, spread = pl.pallas_call(
        functools.partial(kernel, freq_size, sens_size, plan),
        out_shape=(
            jax.ShapeDtypeStruct((rows, sites, step_count), jnp.bfloat16),
            jax.ShapeDtypeStruct((8, LANES), jnp.float32),
        ),
        in_specs=[anywhere] * 7,
        out_specs=(vmem, vmem),
        scratch_shapes=[
            pltpu.VMEM(tiles.shape, jnp.bfloat16),
            pltpu.VMEM(samples.shape, jnp.bfloat16),
            pltpu.VMEM(forward.shape, jnp.bfloat16),
            pltpu.VMEM(inverse.shape, jnp.bfloat16),
            pltpu.SMEM(slot_sensor.shape, jnp.int32),
            pltpu.SMEM(sensor_noise.shape, jnp.float32),
            pltpu.SMEM(advance_offset.shape, jnp.int32),
            pltpu.SemaphoreType.DMA((6,)),
            pltpu.SemaphoreType.DMA((count,)),
            pltpu.VMEM((2, slots, LANES), jnp.float32),
            pltpu.VMEM((slots, wide), jnp.bfloat16),
            pltpu.VMEM((freq_size * 2 * pad, LANES), jnp.float32),
            pltpu.VMEM((freq_size * 2 * pad, LANES), jnp.float32),
            pltpu.VMEM((freq_size * 2 * pad, LANES), jnp.float32),
            pltpu.VMEM((2, freq_size, plan.held_rows, LANES), jnp.bfloat16),
            pltpu.VMEM((lane_tiles, freq_size * chunks * group * 2 * rows, LANES), jnp.float32),
            pltpu.VMEM((freq_size * 2 * m * rows, LANES), jnp.float32),
            pltpu.VMEM((freq_size * 2 * m, rows, LANES), jnp.bfloat16),
            pltpu.VMEM((peers, freq_size * 2 * m, rows, LANES), jnp.bfloat16),
            pltpu.VMEM((2, pad * rows, LANES), jnp.float32),
            pltpu.VMEM((4 * group * pad, rows * SEAT), jnp.bfloat16),
            pltpu.VMEM((rows * SEAT, step_count), jnp.float32),
            pltpu.VMEM((8, LANES), jnp.float32),
            pltpu.VMEM((8, LANES), jnp.float32),
            pltpu.VMEM((peers, 8, LANES), jnp.float32),
            pltpu.SemaphoreType.DMA((count, freq_size - 1)),
            pltpu.SemaphoreType.DMA((count, freq_size - 1)),
            pltpu.SemaphoreType.DMA((peers, freq_size * count)),
            pltpu.SemaphoreType.DMA((peers, freq_size * count)),
            pltpu.SemaphoreType.DMA((peers,)),
            pltpu.SemaphoreType.DMA((peers,)),
        ],
        compiler_params=pltpu.CompilerParams(
            collective_id=0, has_side_effects=True, vmem_limit_bytes=60 * 1024 * 1024
        ),
    )(
        tiles, samples, jnp.asarray(forward, jnp.bfloat16), jnp.asarray(inverse, jnp.bfloat16),
        slot_sensor, sensor_noise, advance_offset,
    )
    noise_spread = spread[0, :sites]
    return (outlook, noise_spread)


def solution(mesh):
    placed = (P("freq", "sens", None), P("freq", None, "sens", None), P("sens"), P(), P())
    return jax.shard_map(
        functools.partial(on_device, mesh.shape["freq"], mesh.shape["sens"]),
        mesh=mesh,
        in_specs=placed,
        out_specs=(P("freq", None, None), P()),
        check_vma=False,
    )
```

```python
import functools
import math

import jax
import jax.numpy as jnp
import numpy as np
from jax import lax
from jax.experimental import pallas as pl
from jax.experimental.pallas import tpu as pltpu
from jax.sharding import PartitionSpec as P

MESH = pl.DeviceIdType.MESH
HALF = 64
LANES = 128
SEAT = 32


class Plan:
    def __init__(self, bins_dev, slots, sites, halves):
        self.bins_dev, self.slots, self.sites = bins_dev, slots, sites
        self.group = HALF // sites
        self.chunks = -(-bins_dev // self.group)
        full = self.chunks // 2
        cut = -(-slots // 32) * 16
        plus = [(c, 0, slots) for c in range(full)]
        minus = [(c, 0, slots) for c in range(self.chunks - full, self.chunks)]
        if self.chunks % 2:
            plus.append((full, 0, cut))
            minus.append((full, cut, slots))
        self.parts = (plus, minus)
        self.m = len(plus)
        self.pad = -(-self.m // 16) * 16
        self.rows = [sum(hi - lo for _, lo, hi in part) for part in self.parts]
        self.held_rows = -(-max(self.rows) // 16) * 16
        ends = [-(-self.m * h // halves) for h in range(halves + 1)]
        self.halves = halves
        self.spans = list(zip(ends[:-1], ends[1:]))
        self.pieces = [(d, h) for h in range(halves) for d in range(2)]

    def size(self, chunk):
        return min(self.group, self.bins_dev - chunk * self.group)

    def row(self, d, k):
        return sum(hi - lo for _, lo, hi in self.parts[d][:k])


def make_tables(freq_size, plan, step_count):
    bins_dev, group, chunks = plan.bins_dev, plan.group, plan.chunks
    period = 2 * freq_size * bins_dev
    slot = np.arange(freq_size * chunks * group)
    block, inside = slot // (chunks * group), slot % (chunks * group)
    live = (inside < bins_dev).astype(np.float64)
    bins = np.where(inside < bins_dev, block * bins_dev + inside, 0)
    turns = bins[:, None] * np.arange(step_count)[None, :] % period
    angle = turns * (2.0 * math.pi / period)
    forward = np.stack([np.cos(angle), -np.sin(angle)]) * live[None, :, None]
    inverse = np.zeros((freq_size, 2, group, 2, plan.pad, step_count))
    weight = (np.where(bins == 0, 1.0, 2.0) / period).reshape(freq_size, chunks, group)
    table = forward.reshape(2, freq_size, chunks, group, step_count) * weight[None, ..., None]
    for d in range(2):
        for k, (chunk, _, _) in enumerate(plan.parts[d]):
            inverse[:, :, :, d, k] = table[:, :, chunk].transpose(1, 0, 2, 3)
    return forward, inverse.reshape(freq_size, 4 * group * plan.pad, step_count)


def kernel(
    freq_size, sens_size, plan,
    tiles_in, samples_in, forward_in, inverse_in, slots_in, noise_in, offsets_in,
    out, spread_out,
    raw, samples, forward, inverse, ids, noise, offsets, load_sem, tile_sem,
    facts, live, cosine, sine, weight,
    held, spectra, z_own, z_send, z_recv, turned_z, gathered, total, staged, spread, spread_send, spread_recv,
    ring_send, ring_recv, z_send_sem, z_recv_sem, s_send_sem, s_recv_sem,
):
    rows, slots, step_count = samples.shape
    n, group, chunks, sites, m, pad = freq_size, plan.group, plan.chunks, plan.sites, plan.m, plan.pad
    bins_dev = plan.bins_dev
    per_bin = 2 * rows
    lane_tiles = spectra.shape[0]
    period = 2 * n * bins_dev
    pieces, halves = plan.pieces, plan.halves
    me_f = lax.axis_index("freq")
    me_s = lax.axis_index("sens")

    def position_of(index):
        odd, pair = lax.rem(index, 2), index // 2
        return pair * (1 - odd) + (n - 1 - pair) * odd

    def index_of(position):
        high = position // (n // 2)
        return 2 * position * (1 - high) + (2 * (n - 1 - position) + 1) * high

    me_p = position_of(me_f)

    def along(step):
        return index_of(lax.rem(me_p + step + 2 * n, n))

    def origin_of(d, arrival):
        return along(arrival if d else -arrival)

    right, left = along(1), along(-1)
    barrier = pltpu.get_barrier_semaphore()
    for neighbour in (left, right):
        pl.semaphore_signal(barrier, inc=1, device_id={"freq": neighbour}, device_id_type=MESH)
    for d in range(1, sens_size):
        peer = lax.rem(me_s + d, sens_size)
        pl.semaphore_signal(barrier, inc=1, device_id={"sens": peer}, device_id_type=MESH)

    tile_loads = []
    for at, (d, h) in enumerate(pieces):
        needed = [
            chunk for chunk, low, high in plan.parts[d][slice(*plan.spans[h])]
            if d == 0 or high - low == slots
        ]
        if needed:
            low = needed[0] * group
            span = pl.ds(low, min((needed[-1] + 1) * group, bins_dev) - low)
            tile_loads.append([pltpu.make_async_copy(tiles_in.at[span], raw.at[span], tile_sem.at[at])])
        else:
            tile_loads.append([])
    loads = [
        pltpu.make_async_copy(source, target, load_sem.at[at])
        for at, (source, target) in enumerate((
            (slots_in, ids), (noise_in, noise), (offsets_in, offsets),
            (forward_in, forward), (samples_in, samples), (inverse_in, inverse),
        ))
    ]
    for load in sum(tile_loads, []) + loads:
        load.start()

    def ring_copy(step, piece, received):
        d, h = piece
        low, high = (plan.row(d, k) for k in plan.spans[h])
        origin = origin_of(d, step + (1 if received else 0))
        block = held.at[d, origin, pl.ds(low, high - low)]
        at = 2 * h + d
        return pltpu.make_async_remote_copy(
            src_ref=block, dst_ref=block,
            send_sem=ring_send.at[at, step], recv_sem=ring_recv.at[at, step],
            device_id={"freq": left if d else right}, device_id_type=MESH,
        )

    line = lax.broadcasted_iota(jnp.int32, (group * sites * 2, LANES), 0)
    spot = lax.broadcasted_iota(jnp.int32, (group * sites * 2, LANES), 1)
    sorter = (spot == lax.rem(line, 2) * HALF + line // 2).astype(jnp.float32).astype(jnp.bfloat16)

    def sort_tiles(d, h):
        for k in range(*plan.spans[h]):
            chunk, low, high = plan.parts[d][k]
            whole = (low, high) == (0, slots)
            if d and not whole:
                continue
            size = plan.size(chunk)
            block = raw[chunk * group:chunk * group + size].reshape(size * sites * 2, slots)
            turned = lax.dot_general(
                block, sorter[:size * sites * 2], (((0,), (0,)), ((), ())),
                preferred_element_type=jnp.float32,
            ).astype(jnp.bfloat16)
            at = plan.row(d, k)
            held[d, me_f, at:at + high - low] = turned[low:high]
            if not whole:
                at = plan.row(1, m - 1)
                held[1, me_f, at:at + slots - high] = turned[high:]

    for at, piece in enumerate(pieces):
        for load in tile_loads[at]:
            load.wait()
        sort_tiles(*piece)
        if at == 0:
            pl.semaphore_wait(barrier, 2 + sens_size - 1)
        ring_copy(0, piece, False).start()

    for load in loads[:3]:
        load.wait()

    def fact(s, carry):
        sensor = ids[s]
        there = (sensor >= 0).astype(jnp.float32)
        facts[0, pl.ds(s, 1), :] = jnp.full((1, LANES), noise[jnp.maximum(sensor, 0)] * there)
        facts[1, pl.ds(s, 1), :] = jnp.full((1, LANES), there)
        return carry

    lax.fori_loop(0, slots, fact, 0, unroll=8)
    there = facts[1].astype(jnp.bfloat16)
    live[...] = jnp.concatenate([there] * (live.shape[1] // LANES), axis=1)
    spread[...] = jnp.zeros_like(spread)
    turned_z[...] = jnp.zeros_like(turned_z)
    total[...] = jnp.zeros_like(total)

    lane = lax.broadcasted_iota(jnp.int32, (rows, LANES), 1)
    which = (lane % HALF) // sites
    sign = jnp.where(lane < HALF, -1.0, 1.0).astype(jnp.float32)

    place = lax.broadcasted_iota(jnp.int32, (2 * pad, LANES), 1)
    seat = lax.broadcasted_iota(jnp.int32, (2 * pad, LANES), 0)
    inside = place % HALF
    lead = jnp.zeros((2 * pad, LANES), jnp.float32)
    for q in range(sites):
        lead = jnp.where(inside % sites == q, offsets[q].astype(jnp.float32), lead)
    side = seat // pad
    chunk_of = jnp.zeros_like(seat)
    for d in range(2):
        for k in range(m):
            chunk_of = jnp.where(seat == d * pad + k, plan.parts[d][k][0], chunk_of)
    within = chunk_of * group + inside // sites
    alive = (within < bins_dev) & (inside < group * sites) & (seat % pad < m)
    turning = 2.0 * math.pi / period

    def phase(arrival, carry):
        block = jnp.where(side == 0, origin_of(0, arrival), origin_of(1, arrival))
        bins = block * bins_dev + within
        ahead = bins.astype(jnp.float32) * lead
        angle = (ahead - period * jnp.floor(ahead / period)) * turning
        here = pl.ds(pl.multiple_of(arrival * 2 * pad, 2 * pad), 2 * pad)
        cosine[here, :] = jnp.cos(angle)
        sine[here, :] = jnp.sin(angle) * jnp.where(place < HALF, -1.0, 1.0)
        weight[here, :] = jnp.where(alive, jnp.where(bins == 0, 1.0, 2.0) / period, 0.0)
        return carry

    lax.fori_loop(0, n, phase, 0)

    def transform(r):
        sample = samples[r] * live[:, :step_count]
        for c in range(2):
            value = lax.dot_general(
                forward[c], sample, (((1,), (1,)), ((), ())),
                preferred_element_type=jnp.float32,
            )
            for tile in range(lane_tiles):
                part = value[:, tile * LANES:min(slots, (tile + 1) * LANES)]
                if part.shape[1] < LANES:
                    part = jnp.concatenate(
                        [part, jnp.zeros((part.shape[0], LANES - part.shape[1]), part.dtype)], axis=1
                    )
                spectra[tile, pl.ds(c * rows + r, part.shape[0], stride=per_bin), :] = part

    def transforms(low, high):
        lax.fori_loop(low, high, lambda r, carry: (transform(r), carry)[1], 0)

    def z_row(arrival, d, k):
        return (arrival * 2 + d) * m + k

    def contract(arrival, piece):
        d, h = piece
        origin = origin_of(d, arrival)
        noisy = spread[...]
        for k in range(*plan.spans[h]):
            chunk, low, high = plan.parts[d][k]
            row = plan.row(d, k)
            weights = held[d, origin, row:row + high - low]
            first = pl.multiple_of((origin * chunks + chunk) * (group * per_bin), group * per_bin)
            parts = [spectra[tile, pl.ds(first, group * per_bin), :] for tile in range(lane_tiles)]
            spec = jnp.concatenate(parts, axis=1)[:, :slots].astype(jnp.bfloat16)
            filled = weights
            if high - low < slots:
                filled = jnp.concatenate(
                    ([jnp.zeros((low, LANES), jnp.bfloat16)] if low else []) + [weights]
                    + ([jnp.zeros((slots - high, LANES), jnp.bfloat16)] if high < slots else []), axis=0
                )
            product = jnp.dot(spec, filled, preferred_element_type=jnp.float32)
            picked = [product[c * rows:(c + 1) * rows] for c in range(2)]
            for i in range(1, group):
                for c in range(2):
                    at = i * per_bin + c * rows
                    picked[c] = jnp.where(which == i, product[at:at + rows], picked[c])
            value = picked[0] + sign * pltpu.roll(picked[1], HALF, 1)
            at = z_row(arrival, d, k)
            z_own[pl.ds(pl.multiple_of(at * rows, rows), rows), :] = value
            z_send[at] = value.astype(jnp.bfloat16)
            wide = weights.astype(jnp.float32)
            power = wide * wide * facts[0, low:high]
            power = power.reshape((high - low) // 8, 8, LANES).sum(axis=0)
            noisy += power * weight[pl.ds(arrival * 2 * pad + d * pad + k, 1), :]
        spread[...] = noisy

    def z_copies(arrival, piece):
        d, h = piece
        low, high = plan.spans[h]
        part = pl.ds(z_row(arrival, d, low), high - low)
        at = arrival * len(pieces) + 2 * h + d
        return [
            pltpu.make_async_remote_copy(
                src_ref=z_send.at[part], dst_ref=z_recv.at[p - 1, part],
                send_sem=z_send_sem.at[p - 1, at], recv_sem=z_recv_sem.at[p - 1, at],
                device_id={"sens": lax.rem(me_s + p, sens_size)}, device_id_type=MESH,
            )
            for p in range(1, sens_size)
        ]

    def send_z(arrival, piece):
        for copy in z_copies(arrival, piece):
            copy.start()

    def receive(step, piece, last=False):
        ring_copy(step, piece, True).wait_recv()
        if not last:
            ring_copy(step + 1, piece, False).start()

    together = LANES // SEAT
    seat_of = lax.broadcasted_iota(jnp.int32, (pad, LANES), 1) // SEAT

    def finish(arrival):
        for piece in pieces:
            for copy in z_copies(arrival, piece):
                copy.wait_recv()
        for d in range(2):
            for k in range(m):
                at = z_row(arrival, d, k)
                value = z_own[pl.ds(pl.multiple_of(at * rows, rows), rows), :]
                for p in range(1, sens_size):
                    value += z_recv[p - 1, at].astype(jnp.float32)
                near = pl.ds(arrival * 2 * pad + d * pad + k, 1)
                turned_z[d, k * rows:(k + 1) * rows] = (
                    value * cosine[near, :] + pltpu.roll(value, HALF, 1) * sine[near, :]
                )
        for d in range(2):
            for base in range(0, rows, together):
                mine = [turned_z[d, pl.ds(base + j, pad, stride=rows), :] for j in range(together)]
                for c in range(2):
                    for i in range(group):
                        start = c * HALF + i * sites
                        value = None
                        for j in range(together):
                            moved = pltpu.roll(mine[j], (j * SEAT - start) % LANES, 1)
                            value = moved if value is None else jnp.where(seat_of == j, moved, value)
                        low = ((c * group + i) * 2 + d) * pad
                        gathered[low:low + pad, base * SEAT:(base + together) * SEAT] = value.astype(jnp.bfloat16)
        origins = [origin_of(d, arrival) for d in range(2)]
        table = jnp.concatenate(
            [
                inverse[origins[d], at * pad:(at + 1) * pad]
                for at, d in ((2 * ci + d, d) for ci in range(2 * group) for d in range(2))
            ], axis=0
        )
        return lax.dot_general(
            gathered[...], table, (((0,), (0,)), ((), ())), preferred_element_type=jnp.float32
        )

    def finished(low, high):
        def one(arrival, carry):
            total[...] += finish(arrival)
            return carry

        lax.fori_loop(low, high, one, 0)

    for load in loads[3:5]:
        load.wait()
    turns = 2 * halves - 1
    early = rows * 5 // 16
    shares = [early + (rows - early) * turn // turns for turn in range(turns + 1)]
    transforms(0, early)

    def contracts(low, high, piece):
        lax.fori_loop(low, high, lambda arrival, carry: (contract(arrival, piece), carry)[1], 0)

    for step in range(2):
        for h in range(halves):
            for d in range(2):
                receive(step, (d, h))
            at = halves * step + h
            if at < turns:
                transforms(shares[at], shares[at + 1])
    loads[5].wait()
    for piece in pieces:
        contracts(0, 2, piece)
        for arrival in range(2):
            send_z(arrival, piece)

    def middle(step, carry):
        for h in range(halves):
            for d in range(2):
                receive(step, (d, h))
            if h == 0:
                for piece in pieces:
                    contract(step, piece)
                    send_z(step, piece)
            if h == halves - 1:
                finished(step - 2, step - 1)
        return carry

    lax.fori_loop(2, n - 2, middle, 0)
    for piece in pieces:
        contract(n - 2, piece)
        send_z(n - 2, piece)
    finished(n - 4, n - 3)
    for h in range(halves):
        for d in range(2):
            receive(n - 2, (d, h), True)
            contract(n - 1, (d, h))
            send_z(n - 1, (d, h))
        if h == 0:
            finished(n - 3, n - 2)
    spread_send[...] = spread[...]
    spread_copies = [
        pltpu.make_async_remote_copy(
            src_ref=spread_send, dst_ref=spread_recv.at[p - 1],
            send_sem=s_send_sem.at[p - 1], recv_sem=s_recv_sem.at[p - 1],
            device_id={"sens": lax.rem(me_s + p, sens_size)}, device_id_type=MESH,
        )
        for p in range(1, sens_size)
    ]
    for copy in spread_copies:
        copy.start()
    for step in range(n - 1):
        for piece in pieces:
            ring_copy(step, piece, False).wait_send()
    for arrival in range(n - 1):
        for piece in pieces:
            for copy in z_copies(arrival, piece):
                copy.wait_send()
    finished(n - 2, n - 1)
    result = total[...] + finish(n - 1)
    for tile in range(staged.shape[0]):
        low, high = tile * LANES, min((tile + 1) * LANES, step_count)
        for r in range(rows):
            staged[tile, pl.ds(r, sites, stride=rows), :high - low] = result[r * SEAT:r * SEAT + sites, low:high]
        for q in range(sites):
            out[q, :, low:high] = staged[tile, q * rows:(q + 1) * rows, :high - low].astype(jnp.bfloat16)
    for copy in spread_copies:
        copy.wait()
    summed = spread[...]
    for p in range(1, sens_size):
        summed += spread_recv[p - 1]
    summed = jnp.broadcast_to(jnp.sum(summed, axis=0, keepdims=True), summed.shape)
    summed = summed + pltpu.roll(summed, HALF, 1)
    folded = summed
    for i in range(1, group):
        folded += pltpu.roll(summed, LANES - i * sites, 1)
    spread_out[...] = folded
    for piece in pieces:
        for copy in z_copies(n - 1, piece):
            copy.wait_send()


def on_device(freq_size, sens_size, samples, response_tiles, slot_sensor, sensor_noise, advance_offset):
    bins_dev, _, slots, sites = response_tiles.shape
    rows, _, step_count = samples.shape
    peers = sens_size - 1
    plan = Plan(bins_dev, slots, sites, 2 if peers * freq_size * 4 <= 1024 else 1)
    group, chunks, m, pad = plan.group, plan.chunks, plan.m, plan.pad
    forward, inverse = make_tables(freq_size, plan, step_count)
    tiles = response_tiles.transpose(0, 3, 1, 2)
    lane_tiles = -(-slots // LANES)
    count = len(plan.pieces)
    wide = -(-step_count // LANES) * LANES
    vmem = pl.BlockSpec(memory_space=pltpu.VMEM)
    anywhere = pl.BlockSpec(memory_space=pl.ANY)
    operands = (
        tiles, samples, jnp.asarray(forward, jnp.bfloat16), jnp.asarray(inverse, jnp.bfloat16),
        slot_sensor, sensor_noise, advance_offset,
    )
    outlook, spread = pl.pallas_call(
        functools.partial(kernel, freq_size, sens_size, plan),
        out_shape=(
            jax.ShapeDtypeStruct((sites, rows, step_count), jnp.bfloat16),
            jax.ShapeDtypeStruct((8, LANES), jnp.float32),
        ),
        in_specs=[anywhere] * 7,
        out_specs=(vmem, vmem),
        scratch_shapes=[
            pltpu.VMEM(tiles.shape, jnp.bfloat16),
            pltpu.VMEM(samples.shape, jnp.bfloat16),
            pltpu.VMEM(forward.shape, jnp.bfloat16),
            pltpu.VMEM(inverse.shape, jnp.bfloat16),
            pltpu.SMEM(slot_sensor.shape, jnp.int32),
            pltpu.SMEM(sensor_noise.shape, jnp.float32),
            pltpu.SMEM(advance_offset.shape, jnp.int32),
            pltpu.SemaphoreType.DMA((6,)),
            pltpu.SemaphoreType.DMA((count,)),
            pltpu.VMEM((2, slots, LANES), jnp.float32),
            pltpu.VMEM((slots, wide), jnp.bfloat16),
            pltpu.VMEM((freq_size * 2 * pad, LANES), jnp.float32),
            pltpu.VMEM((freq_size * 2 * pad, LANES), jnp.float32),
            pltpu.VMEM((freq_size * 2 * pad, LANES), jnp.float32),
            pltpu.VMEM((2, freq_size, plan.held_rows, LANES), jnp.bfloat16),
            pltpu.VMEM((lane_tiles, freq_size * chunks * group * 2 * rows, LANES), jnp.float32),
            pltpu.VMEM((freq_size * 2 * m * rows, LANES), jnp.float32),
            pltpu.VMEM((freq_size * 2 * m, rows, LANES), jnp.bfloat16),
            pltpu.VMEM((peers, freq_size * 2 * m, rows, LANES), jnp.bfloat16),
            pltpu.VMEM((2, pad * rows, LANES), jnp.float32),
            pltpu.VMEM((4 * group * pad, rows * SEAT), jnp.bfloat16),
            pltpu.VMEM((rows * SEAT, step_count), jnp.float32),
            pltpu.VMEM((wide // LANES, sites * rows, LANES), jnp.float32),
            pltpu.VMEM((8, LANES), jnp.float32),
            pltpu.VMEM((8, LANES), jnp.float32),
            pltpu.VMEM((peers, 8, LANES), jnp.float32),
            pltpu.SemaphoreType.DMA((count, freq_size - 1)),
            pltpu.SemaphoreType.DMA((count, freq_size - 1)),
            pltpu.SemaphoreType.DMA((peers, freq_size * count)),
            pltpu.SemaphoreType.DMA((peers, freq_size * count)),
            pltpu.SemaphoreType.DMA((peers,)),
            pltpu.SemaphoreType.DMA((peers,)),
        ],
        compiler_params=pltpu.CompilerParams(
            collective_id=0, has_side_effects=True, vmem_limit_bytes=50 * 1024 * 1024
        ),
    )(*(pltpu.with_memory_space_constraint(array, pltpu.HBM) for array in operands))
    noise_spread = spread[0, :sites]
    return (outlook.transpose(1, 0, 2), noise_spread)


def solution(mesh):
    placed = (P("freq", "sens", None), P("freq", None, "sens", None), P("sens"), P(), P())
    return jax.shard_map(
        functools.partial(on_device, mesh.shape["freq"], mesh.shape["sens"]),
        mesh=mesh,
        in_specs=placed,
        out_specs=(P("freq", None, None), P()),
        check_vma=False,
    )
```

```python
import functools
import math

import jax
import jax.numpy as jnp
import numpy as np
from jax import lax
from jax.experimental import pallas as pl
from jax.experimental.pallas import tpu as pltpu
from jax.sharding import PartitionSpec as P

MESH = pl.DeviceIdType.MESH
HALF = 64
LANES = 128
SEAT = 32


class Plan:
    def __init__(self, bins_dev, slots, sites, halves):
        self.bins_dev, self.slots, self.sites = bins_dev, slots, sites
        self.group = HALF // sites
        self.chunks = -(-bins_dev // self.group)
        full = self.chunks // 2
        cut = -(-slots // 32) * 16
        plus = [(c, 0, slots) for c in range(full)]
        minus = [(c, 0, slots) for c in range(self.chunks - full, self.chunks)]
        if self.chunks % 2:
            plus.append((full, 0, cut))
            minus.append((full, cut, slots))
        self.parts = (plus, minus)
        self.m = len(plus)
        self.pad = -(-self.m // 16) * 16
        self.rows = [sum(hi - lo for _, lo, hi in part) for part in self.parts]
        self.held_rows = -(-max(self.rows) // 16) * 16
        ends = [-(-self.m * h // halves) for h in range(halves + 1)]
        self.halves = halves
        self.spans = list(zip(ends[:-1], ends[1:]))
        self.pieces = [(d, h) for h in range(halves) for d in range(2)]

    def size(self, chunk):
        return min(self.group, self.bins_dev - chunk * self.group)

    def row(self, d, k):
        return sum(hi - lo for _, lo, hi in self.parts[d][:k])


def make_tables(freq_size, plan, step_count):
    bins_dev, group, chunks = plan.bins_dev, plan.group, plan.chunks
    period = 2 * freq_size * bins_dev
    slot = np.arange(freq_size * chunks * group)
    block, inside = slot // (chunks * group), slot % (chunks * group)
    live = (inside < bins_dev).astype(np.float64)
    bins = np.where(inside < bins_dev, block * bins_dev + inside, 0)
    turns = bins[:, None] * np.arange(step_count)[None, :] % period
    angle = turns * (2.0 * math.pi / period)
    forward = np.stack([np.cos(angle), -np.sin(angle)]) * live[None, :, None]
    inverse = np.zeros((freq_size, 2, group, 2, plan.pad, step_count))
    weight = (np.where(bins == 0, 1.0, 2.0) / period).reshape(freq_size, chunks, group)
    table = forward.reshape(2, freq_size, chunks, group, step_count) * weight[None, ..., None]
    for d in range(2):
        for k, (chunk, _, _) in enumerate(plan.parts[d]):
            inverse[:, :, :, d, k] = table[:, :, chunk].transpose(1, 0, 2, 3)
    return forward, inverse.reshape(freq_size, 4 * group * plan.pad, step_count)


def kernel(
    freq_size, sens_size, plan,
    tiles_in, samples_in, forward_in, inverse_in, slots_in, noise_in, offsets_in,
    out, spread_out,
    raw, samples, forward, inverse, ids, noise, offsets, load_sem, tile_sem,
    facts, live, cosine, sine, weight,
    held, spectra, z_own, z_send, z_recv, turned_z, gathered, total, staged, spread, spread_send, spread_recv,
    ring_send, ring_recv, z_send_sem, z_recv_sem, s_send_sem, s_recv_sem,
):
    rows, slots, step_count = samples.shape
    n, group, chunks, sites, m, pad = freq_size, plan.group, plan.chunks, plan.sites, plan.m, plan.pad
    bins_dev = plan.bins_dev
    per_bin = 2 * rows
    lane_tiles = spectra.shape[0]
    period = 2 * n * bins_dev
    pieces, halves = plan.pieces, plan.halves
    me_f = lax.axis_index("freq")
    me_s = lax.axis_index("sens")

    def position_of(index):
        odd, pair = lax.rem(index, 2), index // 2
        return pair * (1 - odd) + (n - 1 - pair) * odd

    def index_of(position):
        high = position // (n // 2)
        return 2 * position * (1 - high) + (2 * (n - 1 - position) + 1) * high

    me_p = position_of(me_f)

    def along(step):
        return index_of(lax.rem(me_p + step + 2 * n, n))

    def origin_of(d, arrival):
        return along(arrival if d else -arrival)

    right, left = along(1), along(-1)
    barrier = pltpu.get_barrier_semaphore()
    for neighbour in (left, right):
        pl.semaphore_signal(barrier, inc=1, device_id={"freq": neighbour}, device_id_type=MESH)
    for d in range(1, sens_size):
        peer = lax.rem(me_s + d, sens_size)
        pl.semaphore_signal(barrier, inc=1, device_id={"sens": peer}, device_id_type=MESH)

    tile_loads = []
    for at, (d, h) in enumerate(pieces):
        needed = [
            chunk for chunk, low, high in plan.parts[d][slice(*plan.spans[h])]
            if d == 0 or high - low == slots
        ]
        if needed:
            low = needed[0] * group
            span = pl.ds(low, min((needed[-1] + 1) * group, bins_dev) - low)
            tile_loads.append([pltpu.make_async_copy(tiles_in.at[span], raw.at[span], tile_sem.at[at])])
        else:
            tile_loads.append([])
    loads = [
        pltpu.make_async_copy(source, target, load_sem.at[at])
        for at, (source, target) in enumerate((
            (slots_in, ids), (noise_in, noise), (offsets_in, offsets),
            (forward_in, forward), (samples_in, samples), (inverse_in, inverse),
        ))
    ]
    for load in sum(tile_loads, []) + loads:
        load.start()

    def ring_copy(step, piece, received):
        d, h = piece
        low, high = (plan.row(d, k) for k in plan.spans[h])
        origin = origin_of(d, step + (1 if received else 0))
        block = held.at[d, origin, pl.ds(low, high - low)]
        at = 2 * h + d
        return pltpu.make_async_remote_copy(
            src_ref=block, dst_ref=block,
            send_sem=ring_send.at[d], recv_sem=ring_recv.at[at, step],
            device_id={"freq": left if d else right}, device_id_type=MESH,
        )

    line = lax.broadcasted_iota(jnp.int32, (group * sites * 2, LANES), 0)
    spot = lax.broadcasted_iota(jnp.int32, (group * sites * 2, LANES), 1)
    sorter = (spot == lax.rem(line, 2) * HALF + line // 2).astype(jnp.float32).astype(jnp.bfloat16)

    def sort_tiles(d, h):
        for k in range(*plan.spans[h]):
            chunk, low, high = plan.parts[d][k]
            whole = (low, high) == (0, slots)
            if d and not whole:
                continue
            size = plan.size(chunk)
            block = raw[chunk * group:chunk * group + size].reshape(size * sites * 2, slots)
            turned = lax.dot_general(
                block, sorter[:size * sites * 2], (((0,), (0,)), ((), ())),
                preferred_element_type=jnp.float32,
            ).astype(jnp.bfloat16)
            at = plan.row(d, k)
            held[d, me_f, at:at + high - low] = turned[low:high]
            if not whole:
                at = plan.row(1, m - 1)
                held[1, me_f, at:at + slots - high] = turned[high:]

    for at, piece in enumerate(pieces):
        for load in tile_loads[at]:
            load.wait()
        sort_tiles(*piece)
        if at == 0:
            pl.semaphore_wait(barrier, 2 + sens_size - 1)
        ring_copy(0, piece, False).start()

    for load in loads[:3]:
        load.wait()

    def fact(s, carry):
        sensor = ids[s]
        there = (sensor >= 0).astype(jnp.float32)
        facts[0, pl.ds(s, 1), :] = jnp.full((1, LANES), noise[jnp.maximum(sensor, 0)] * there)
        facts[1, pl.ds(s, 1), :] = jnp.full((1, LANES), there)
        return carry

    lax.fori_loop(0, slots, fact, 0, unroll=8)
    there = facts[1].astype(jnp.bfloat16)
    live[...] = jnp.concatenate([there] * (live.shape[1] // LANES), axis=1)
    spread[...] = jnp.zeros_like(spread)
    turned_z[...] = jnp.zeros_like(turned_z)
    total[...] = jnp.zeros_like(total)

    lane = lax.broadcasted_iota(jnp.int32, (rows, LANES), 1)
    which = (lane % HALF) // sites
    sign = jnp.where(lane < HALF, -1.0, 1.0).astype(jnp.float32)

    place = lax.broadcasted_iota(jnp.int32, (2 * pad, LANES), 1)
    seat = lax.broadcasted_iota(jnp.int32, (2 * pad, LANES), 0)
    inside = place % HALF
    lead = jnp.zeros((2 * pad, LANES), jnp.float32)
    for q in range(sites):
        lead = jnp.where(inside % sites == q, offsets[q].astype(jnp.float32), lead)
    side = seat // pad
    chunk_of = jnp.zeros_like(seat)
    for d in range(2):
        for k in range(m):
            chunk_of = jnp.where(seat == d * pad + k, plan.parts[d][k][0], chunk_of)
    within = chunk_of * group + inside // sites
    alive = (within < bins_dev) & (inside < group * sites) & (seat % pad < m)
    turning = 2.0 * math.pi / period

    def phase(arrival, carry):
        block = jnp.where(side == 0, origin_of(0, arrival), origin_of(1, arrival))
        bins = block * bins_dev + within
        ahead = bins.astype(jnp.float32) * lead
        angle = (ahead - period * jnp.floor(ahead / period)) * turning
        here = pl.ds(pl.multiple_of(arrival * 2 * pad, 2 * pad), 2 * pad)
        cosine[here, :] = jnp.cos(angle)
        sine[here, :] = jnp.sin(angle) * jnp.where(place < HALF, -1.0, 1.0)
        weight[here, :] = jnp.where(alive, jnp.where(bins == 0, 1.0, 2.0) / period, 0.0)
        return carry

    lax.fori_loop(0, n, phase, 0)

    def transform(r):
        sample = samples[r] * live[:, :step_count]
        for c in range(2):
            value = lax.dot_general(
                forward[c], sample, (((1,), (1,)), ((), ())),
                preferred_element_type=jnp.float32,
            )
            for tile in range(lane_tiles):
                part = value[:, tile * LANES:min(slots, (tile + 1) * LANES)]
                if part.shape[1] < LANES:
                    part = jnp.concatenate(
                        [part, jnp.zeros((part.shape[0], LANES - part.shape[1]), part.dtype)], axis=1
                    )
                spectra[tile, pl.ds(c * rows + r, part.shape[0], stride=per_bin), :] = part

    def transforms(low, high):
        lax.fori_loop(low, high, lambda r, carry: (transform(r), carry)[1], 0)

    def z_row(arrival, d, k):
        return (arrival * 2 + d) * m + k

    def contract(arrival, piece):
        d, h = piece
        origin = origin_of(d, arrival)
        noisy = spread[...]
        for k in range(*plan.spans[h]):
            chunk, low, high = plan.parts[d][k]
            row = plan.row(d, k)
            weights = held[d, origin, row:row + high - low]
            first = pl.multiple_of((origin * chunks + chunk) * (group * per_bin), group * per_bin)
            parts = [spectra[tile, pl.ds(first, group * per_bin), :] for tile in range(lane_tiles)]
            spec = jnp.concatenate(parts, axis=1)[:, :slots].astype(jnp.bfloat16)
            filled = weights
            if high - low < slots:
                filled = jnp.concatenate(
                    ([jnp.zeros((low, LANES), jnp.bfloat16)] if low else []) + [weights]
                    + ([jnp.zeros((slots - high, LANES), jnp.bfloat16)] if high < slots else []), axis=0
                )
            product = jnp.dot(spec, filled, preferred_element_type=jnp.float32)
            picked = [product[c * rows:(c + 1) * rows] for c in range(2)]
            for i in range(1, group):
                for c in range(2):
                    at = i * per_bin + c * rows
                    picked[c] = jnp.where(which == i, product[at:at + rows], picked[c])
            value = picked[0] + sign * pltpu.roll(picked[1], HALF, 1)
            at = z_row(arrival, d, k)
            z_own[pl.ds(pl.multiple_of(at * rows, rows), rows), :] = value
            z_send[at] = value.astype(jnp.bfloat16)
            wide = weights.astype(jnp.float32)
            power = wide * wide * facts[0, low:high]
            power = power.reshape((high - low) // 8, 8, LANES).sum(axis=0)
            noisy += power * weight[pl.ds(arrival * 2 * pad + d * pad + k, 1), :]
        spread[...] = noisy

    def z_copies(arrival, piece):
        d, h = piece
        low, high = plan.spans[h]
        part = pl.ds(z_row(arrival, d, low), high - low)
        return [
            pltpu.make_async_remote_copy(
                src_ref=z_send.at[part], dst_ref=z_recv.at[p - 1, part],
                send_sem=z_send_sem.at[0], recv_sem=z_recv_sem.at[arrival],
                device_id={"sens": lax.rem(me_s + p, sens_size)}, device_id_type=MESH,
            )
            for p in range(1, sens_size)
        ]

    def send_z(arrival, piece):
        for copy in z_copies(arrival, piece):
            copy.start()

    def receive(step, piece, last=False):
        ring_copy(step, piece, True).wait_recv()
        if not last:
            ring_copy(step + 1, piece, False).start()

    together = LANES // SEAT
    seat_of = lax.broadcasted_iota(jnp.int32, (pad, LANES), 1) // SEAT

    def finish(arrival):
        landed = z_recv.at[:, pl.ds(z_row(arrival, 0, 0), 2 * m)]
        pltpu.make_async_copy(landed, landed, z_recv_sem.at[arrival]).wait()
        for d in range(2):
            for k in range(m):
                at = z_row(arrival, d, k)
                value = z_own[pl.ds(pl.multiple_of(at * rows, rows), rows), :]
                for p in range(1, sens_size):
                    value += z_recv[p - 1, at].astype(jnp.float32)
                near = pl.ds(arrival * 2 * pad + d * pad + k, 1)
                turned_z[d, k * rows:(k + 1) * rows] = (
                    value * cosine[near, :] + pltpu.roll(value, HALF, 1) * sine[near, :]
                )
        for d in range(2):
            for base in range(0, rows, together):
                mine = [turned_z[d, pl.ds(base + j, pad, stride=rows), :] for j in range(together)]
                for c in range(2):
                    for i in range(group):
                        start = c * HALF + i * sites
                        value = None
                        for j in range(together):
                            moved = pltpu.roll(mine[j], (j * SEAT - start) % LANES, 1)
                            value = moved if value is None else jnp.where(seat_of == j, moved, value)
                        low = ((c * group + i) * 2 + d) * pad
                        gathered[low:low + pad, base * SEAT:(base + together) * SEAT] = value.astype(jnp.bfloat16)
        origins = [origin_of(d, arrival) for d in range(2)]
        table = jnp.concatenate(
            [
                inverse[origins[d], at * pad:(at + 1) * pad]
                for at, d in ((2 * ci + d, d) for ci in range(2 * group) for d in range(2))
            ], axis=0
        )
        return lax.dot_general(
            gathered[...], table, (((0,), (0,)), ((), ())), preferred_element_type=jnp.float32
        )

    def finished(low, high):
        def one(arrival, carry):
            total[...] += finish(arrival)
            return carry

        lax.fori_loop(low, high, one, 0)

    for load in loads[3:5]:
        load.wait()
    turns = 2 * halves - 1
    early = rows * 5 // 16
    shares = [early + (rows - early) * turn // turns for turn in range(turns + 1)]
    transforms(0, early)

    def contracts(low, high, piece):
        lax.fori_loop(low, high, lambda arrival, carry: (contract(arrival, piece), carry)[1], 0)

    for step in range(2):
        for h in range(halves):
            for d in range(2):
                receive(step, (d, h))
            at = halves * step + h
            if at < turns:
                transforms(shares[at], shares[at + 1])
    loads[5].wait()
    for piece in pieces:
        contracts(0, 2, piece)
        for arrival in range(2):
            send_z(arrival, piece)

    def middle(step, carry):
        for h in range(halves):
            for d in range(2):
                receive(step, (d, h))
            if h == 0:
                for piece in pieces:
                    contract(step, piece)
                    send_z(step, piece)
            if h == halves - 1:
                finished(step - 2, step - 1)
        return carry

    lax.fori_loop(2, n - 2, middle, 0)
    for piece in pieces:
        contract(n - 2, piece)
        send_z(n - 2, piece)
    finished(n - 4, n - 3)
    for h in range(halves):
        for d in range(2):
            receive(n - 2, (d, h), True)
            contract(n - 1, (d, h))
            send_z(n - 1, (d, h))
        if h == 0:
            finished(n - 3, n - 2)
    spread_send[...] = spread[...]
    spread_copies = [
        pltpu.make_async_remote_copy(
            src_ref=spread_send, dst_ref=spread_recv.at[p - 1],
            send_sem=s_send_sem.at[0], recv_sem=s_recv_sem.at[0],
            device_id={"sens": lax.rem(me_s + p, sens_size)}, device_id_type=MESH,
        )
        for p in range(1, sens_size)
    ]
    for copy in spread_copies:
        copy.start()
    for d in range(2):
        gone = held.at[d, pl.ds(0, n - 1), pl.ds(0, plan.rows[d])]
        pltpu.make_async_copy(gone, gone, ring_send.at[d]).wait()
    finished(n - 2, n - 1)
    result = total[...] + finish(n - 1)
    for tile in range(staged.shape[0]):
        low, high = tile * LANES, min((tile + 1) * LANES, step_count)
        for r in range(rows):
            staged[tile, pl.ds(r, sites, stride=rows), :high - low] = result[r * SEAT:r * SEAT + sites, low:high]
        for q in range(sites):
            out[q, :, low:high] = staged[tile, q * rows:(q + 1) * rows, :high - low].astype(jnp.bfloat16)
    pltpu.make_async_copy(spread_recv, spread_recv, s_send_sem.at[0]).wait()
    pltpu.make_async_copy(spread_recv, spread_recv, s_recv_sem.at[0]).wait()
    summed = spread[...]
    for p in range(1, sens_size):
        summed += spread_recv[p - 1]
    summed = jnp.broadcast_to(jnp.sum(summed, axis=0, keepdims=True), summed.shape)
    summed = summed + pltpu.roll(summed, HALF, 1)
    folded = summed
    for i in range(1, group):
        folded += pltpu.roll(summed, LANES - i * sites, 1)
    spread_out[...] = folded
    pltpu.make_async_copy(z_recv, z_recv, z_send_sem.at[0]).wait()


def on_device(freq_size, sens_size, samples, response_tiles, slot_sensor, sensor_noise, advance_offset):
    bins_dev, _, slots, sites = response_tiles.shape
    rows, _, step_count = samples.shape
    peers = sens_size - 1
    plan = Plan(bins_dev, slots, sites, 2)
    group, chunks, m, pad = plan.group, plan.chunks, plan.m, plan.pad
    forward, inverse = make_tables(freq_size, plan, step_count)
    tiles = response_tiles.transpose(0, 3, 1, 2)
    lane_tiles = -(-slots // LANES)
    count = len(plan.pieces)
    wide = -(-step_count // LANES) * LANES
    vmem = pl.BlockSpec(memory_space=pltpu.VMEM)
    anywhere = pl.BlockSpec(memory_space=pl.ANY)
    operands = (
        tiles, samples, jnp.asarray(forward, jnp.bfloat16), jnp.asarray(inverse, jnp.bfloat16),
        slot_sensor, sensor_noise, advance_offset,
    )
    outlook, spread = pl.pallas_call(
        functools.partial(kernel, freq_size, sens_size, plan),
        out_shape=(
            jax.ShapeDtypeStruct((sites, rows, step_count), jnp.bfloat16),
            jax.ShapeDtypeStruct((8, LANES), jnp.float32),
        ),
        in_specs=[anywhere] * 7,
        out_specs=(vmem, vmem),
        scratch_shapes=[
            pltpu.VMEM(tiles.shape, jnp.bfloat16),
            pltpu.VMEM(samples.shape, jnp.bfloat16),
            pltpu.VMEM(forward.shape, jnp.bfloat16),
            pltpu.VMEM(inverse.shape, jnp.bfloat16),
            pltpu.SMEM(slot_sensor.shape, jnp.int32),
            pltpu.SMEM(sensor_noise.shape, jnp.float32),
            pltpu.SMEM(advance_offset.shape, jnp.int32),
            pltpu.SemaphoreType.DMA((6,)),
            pltpu.SemaphoreType.DMA((count,)),
            pltpu.VMEM((2, slots, LANES), jnp.float32),
            pltpu.VMEM((slots, wide), jnp.bfloat16),
            pltpu.VMEM((freq_size * 2 * pad, LANES), jnp.float32),
            pltpu.VMEM((freq_size * 2 * pad, LANES), jnp.float32),
            pltpu.VMEM((freq_size * 2 * pad, LANES), jnp.float32),
            pltpu.VMEM((2, freq_size, plan.held_rows, LANES), jnp.bfloat16),
            pltpu.VMEM((lane_tiles, freq_size * chunks * group * 2 * rows, LANES), jnp.float32),
            pltpu.VMEM((freq_size * 2 * m * rows, LANES), jnp.float32),
            pltpu.VMEM((freq_size * 2 * m, rows, LANES), jnp.bfloat16),
            pltpu.VMEM((peers, freq_size * 2 * m, rows, LANES), jnp.bfloat16),
            pltpu.VMEM((2, pad * rows, LANES), jnp.float32),
            pltpu.VMEM((4 * group * pad, rows * SEAT), jnp.bfloat16),
            pltpu.VMEM((rows * SEAT, step_count), jnp.float32),
            pltpu.VMEM((wide // LANES, sites * rows, LANES), jnp.float32),
            pltpu.VMEM((8, LANES), jnp.float32),
            pltpu.VMEM((8, LANES), jnp.float32),
            pltpu.VMEM((peers, 8, LANES), jnp.float32),
            pltpu.SemaphoreType.DMA((2,)),
            pltpu.SemaphoreType.DMA((count, freq_size - 1)),
            pltpu.SemaphoreType.DMA((1,)),
            pltpu.SemaphoreType.DMA((freq_size,)),
            pltpu.SemaphoreType.DMA((1,)),
            pltpu.SemaphoreType.DMA((1,)),
        ],
        compiler_params=pltpu.CompilerParams(
            collective_id=0, has_side_effects=True, vmem_limit_bytes=50 * 1024 * 1024
        ),
    )(*(pltpu.with_memory_space_constraint(array, pltpu.HBM) for array in operands))
    noise_spread = spread[0, :sites]
    return (outlook.transpose(1, 0, 2), noise_spread)


def solution(mesh):
    placed = (P("freq", "sens", None), P("freq", None, "sens", None), P("sens"), P(), P())
    return jax.shard_map(
        functools.partial(on_device, mesh.shape["freq"], mesh.shape["sens"]),
        mesh=mesh,
        in_specs=placed,
        out_specs=(P("freq", None, None), P()),
        check_vma=False,
    )
```

```python
import functools
import math

import jax
import jax.numpy as jnp
import numpy as np
from jax import lax
from jax.experimental import pallas as pl
from jax.experimental.pallas import tpu as pltpu
from jax.sharding import PartitionSpec as P

MESH = pl.DeviceIdType.MESH
HALF = 64
LANES = 128
SEAT = 32


class Plan:
    def __init__(self, bins_dev, slots, sites):
        self.bins_dev, self.slots, self.sites = bins_dev, slots, sites
        self.group = HALF // sites
        self.chunks = -(-bins_dev // self.group)
        full = self.chunks // 2
        last = self.chunks - 1
        loose = self.group == 3 and bins_dev - last * 3 == 2 and last > 0
        self.moved = slots // 24 * 8 if loose else 0
        self.kept = slots - self.moved
        cut = (self.kept + 16) // 32 * 16
        plus = [(c, 0, slots) for c in range(full)]
        minus = [(c, 0, slots) for c in range(self.chunks - full, self.chunks)]
        if self.chunks % 2:
            plus.append((full, 0, cut))
            minus.append((full, cut, slots))
        self.parts = (plus, minus)
        self.m = len(plus)
        self.pad = -(-self.m // 16) * 16
        self.rows = [sum(map(self.height, part)) for part in self.parts]
        self.held_rows = -(-max(self.rows) // 16) * 16
        ends = sorted({0, -(-self.m * 3 // 10), -(-self.m * 7 // 10), self.m})
        self.halves = halves = len(ends) - 1
        self.spans = list(zip(ends[:-1], ends[1:]))
        self.pieces = [(d, h) for h in range(halves) for d in range(2)]

    def size(self, chunk):
        return min(self.group, self.bins_dev - chunk * self.group)

    def packed(self, chunk):
        return self.moved > 0 and chunk == self.chunks - 1

    def height(self, entry):
        chunk, low, high = entry
        return self.kept if self.packed(chunk) else high - low

    def row(self, d, k):
        return sum(map(self.height, self.parts[d][:k]))


def make_tables(freq_size, plan, step_count):
    bins_dev, group, chunks = plan.bins_dev, plan.group, plan.chunks
    period = 2 * freq_size * bins_dev
    slot = np.arange(freq_size * chunks * group)
    block, inside = slot // (chunks * group), slot % (chunks * group)
    live = (inside < bins_dev).astype(np.float64)
    bins = np.where(inside < bins_dev, block * bins_dev + inside, 0)
    turns = bins[:, None] * np.arange(step_count)[None, :] % period
    angle = turns * (2.0 * math.pi / period)
    forward = np.stack([np.cos(angle), -np.sin(angle)]) * live[None, :, None]
    inverse = np.zeros((freq_size, 2, group, 2, plan.pad, step_count))
    weight = (np.where(bins == 0, 1.0, 2.0) / period).reshape(freq_size, chunks, group)
    table = forward.reshape(2, freq_size, chunks, group, step_count) * weight[None, ..., None]
    for d in range(2):
        for k, (chunk, _, _) in enumerate(plan.parts[d]):
            inverse[:, :, :, d, k] = table[:, :, chunk].transpose(1, 0, 2, 3)
    return forward, inverse.reshape(freq_size, 4 * group * plan.pad, step_count)


def kernel(
    freq_size, sens_size, plan,
    tiles_in, samples_in, forward_in, inverse_in, slots_in, noise_in, offsets_in,
    out, spread_out,
    raw, samples, forward, inverse, ids, noise, offsets, load_sem, tile_sem,
    facts, facts_packed, live, cosine, sine, weight,
    held, spectra, z_own, z_send, z_recv, turned_z, gathered, total, staged, spread, spread_send, spread_recv,
    ring_send, ring_recv, z_send_sem, z_recv_sem, s_send_sem, s_recv_sem,
):
    rows, slots, step_count = samples.shape
    n, group, chunks, sites, m, pad = freq_size, plan.group, plan.chunks, plan.sites, plan.m, plan.pad
    bins_dev, kept, moved = plan.bins_dev, plan.kept, plan.moved
    per_bin = 2 * rows
    lane_tiles = spectra.shape[0]
    period = 2 * n * bins_dev
    pieces, halves = plan.pieces, plan.halves
    me_f = lax.axis_index("freq")
    me_s = lax.axis_index("sens")

    def position_of(index):
        odd, pair = lax.rem(index, 2), index // 2
        return pair * (1 - odd) + (n - 1 - pair) * odd

    def index_of(position):
        high = position // (n // 2)
        return 2 * position * (1 - high) + (2 * (n - 1 - position) + 1) * high

    me_p = position_of(me_f)

    def along(step):
        return index_of(lax.rem(me_p + step + 2 * n, n))

    def origin_of(d, arrival):
        return along(arrival if d else -arrival)

    right, left = along(1), along(-1)
    barrier = pltpu.get_barrier_semaphore()
    for neighbour in (left, right):
        pl.semaphore_signal(barrier, inc=1, device_id={"freq": neighbour}, device_id_type=MESH)
    for d in range(1, sens_size):
        peer = lax.rem(me_s + d, sens_size)
        pl.semaphore_signal(barrier, inc=1, device_id={"sens": peer}, device_id_type=MESH)

    tile_loads = []
    for at, (d, h) in enumerate(pieces):
        needed = [
            chunk for chunk, low, high in plan.parts[d][slice(*plan.spans[h])]
            if d == 0 or high - low == slots
        ]
        if needed:
            low = needed[0] * group
            span = pl.ds(low, min((needed[-1] + 1) * group, bins_dev) - low)
            tile_loads.append([pltpu.make_async_copy(tiles_in.at[span], raw.at[span], tile_sem.at[at])])
        else:
            tile_loads.append([])
    loads = [
        pltpu.make_async_copy(source, target, load_sem.at[at])
        for at, (source, target) in enumerate((
            (slots_in, ids), (noise_in, noise), (offsets_in, offsets),
            (forward_in, forward), (samples_in, samples), (inverse_in, inverse),
        ))
    ]
    for load in sum(tile_loads, []) + loads:
        load.start()

    def ring_copy(step, piece, received):
        d, h = piece
        low, high = (plan.row(d, k) for k in plan.spans[h])
        origin = origin_of(d, step + (1 if received else 0))
        block = held.at[d, origin, pl.ds(low, high - low)]
        at = 2 * h + d
        return pltpu.make_async_remote_copy(
            src_ref=block, dst_ref=block,
            send_sem=ring_send.at[d], recv_sem=ring_recv.at[at, step],
            device_id={"freq": left if d else right}, device_id_type=MESH,
        )

    line = lax.broadcasted_iota(jnp.int32, (group * sites * 2, LANES), 0)
    spot = lax.broadcasted_iota(jnp.int32, (group * sites * 2, LANES), 1)
    sorter = (spot == lax.rem(line, 2) * HALF + line // 2).astype(jnp.float32).astype(jnp.bfloat16)

    def sort_tiles(d, h):
        for k in range(*plan.spans[h]):
            chunk, low, high = plan.parts[d][k]
            whole = (low, high) == (0, slots)
            if d and not whole:
                continue
            size = plan.size(chunk)
            block = raw[chunk * group:chunk * group + size].reshape(size * sites * 2, slots)
            turned = lax.dot_general(
                block, sorter[:size * sites * 2], (((0,), (0,)), ((), ())),
                preferred_element_type=jnp.float32,
            ).astype(jnp.bfloat16)
            at = plan.row(d, k)
            if plan.packed(chunk):
                aside = []
                for i in range(size):
                    one = raw[chunk * group + i].reshape(sites * 2, slots)
                    aside.append(lax.dot_general(
                        one, sorter[size * sites * 2:], (((0,), (0,)), ((), ())),
                        preferred_element_type=jnp.float32,
                    )[kept:])
                aside.append(jnp.zeros((kept - size * moved, LANES), jnp.float32))
                both = turned[:kept].astype(jnp.float32) + jnp.concatenate(aside, axis=0)
                held[d, me_f, at:at + kept] = both.astype(jnp.bfloat16)
                continue
            held[d, me_f, at:at + high - low] = turned[low:high]
            if not whole:
                at = plan.row(1, m - 1)
                held[1, me_f, at:at + slots - high] = turned[high:]

    for at, piece in enumerate(pieces):
        for load in tile_loads[at]:
            load.wait()
        sort_tiles(*piece)
        if at == 0:
            pl.semaphore_wait(barrier, 2 + sens_size - 1)
        ring_copy(0, piece, False).start()

    for load in loads[:3]:
        load.wait()

    def fact(s, carry):
        sensor = ids[s]
        there = (sensor >= 0).astype(jnp.float32)
        facts[0, pl.ds(s, 1), :] = jnp.full((1, LANES), noise[jnp.maximum(sensor, 0)] * there)
        facts[1, pl.ds(s, 1), :] = jnp.full((1, LANES), there)
        return carry

    lax.fori_loop(0, slots, fact, 0, unroll=8)
    if moved:
        aside = [facts[0, kept:]] * (group - 1) + [jnp.zeros((kept - (group - 1) * moved, LANES), jnp.float32)]
        spare = lax.broadcasted_iota(jnp.int32, (kept, LANES), 1) % HALF // sites == group - 1
        facts_packed[...] = jnp.where(spare, jnp.concatenate(aside, axis=0), facts[0, :kept])
    there = facts[1].astype(jnp.bfloat16)
    live[...] = jnp.concatenate([there] * (live.shape[1] // LANES), axis=1)
    spread[...] = jnp.zeros_like(spread)
    turned_z[...] = jnp.zeros_like(turned_z)
    total[...] = jnp.zeros_like(total)

    lane = lax.broadcasted_iota(jnp.int32, (rows, LANES), 1)
    which = (lane % HALF) // sites
    sign = jnp.where(lane < HALF, -1.0, 1.0).astype(jnp.float32)

    place = lax.broadcasted_iota(jnp.int32, (2 * pad, LANES), 1)
    seat = lax.broadcasted_iota(jnp.int32, (2 * pad, LANES), 0)
    inside = place % HALF
    lead = jnp.zeros((2 * pad, LANES), jnp.float32)
    for q in range(sites):
        lead = jnp.where(inside % sites == q, offsets[q].astype(jnp.float32), lead)
    side = seat // pad
    chunk_of = jnp.zeros_like(seat)
    for d in range(2):
        for k in range(m):
            chunk_of = jnp.where(seat == d * pad + k, plan.parts[d][k][0], chunk_of)
    within = chunk_of * group + inside // sites
    alive = (within < bins_dev) & (inside < group * sites) & (seat % pad < m)
    turning = 2.0 * math.pi / period
    seats = [d * pad + k for d in range(2) for k in range(m) if plan.packed(plan.parts[d][k][0])]
    extra = jnp.zeros((2 * pad, LANES), jnp.float32)
    for row in seats:
        extra = jnp.where((seat == row) & (inside // sites == group - 1), 2.0 / period, extra)

    def phase(arrival, carry):
        block = jnp.where(side == 0, origin_of(0, arrival), origin_of(1, arrival))
        bins = block * bins_dev + within
        ahead = bins.astype(jnp.float32) * lead
        angle = (ahead - period * jnp.floor(ahead / period)) * turning
        here = pl.ds(pl.multiple_of(arrival * 2 * pad, 2 * pad), 2 * pad)
        cosine[here, :] = jnp.cos(angle)
        sine[here, :] = jnp.sin(angle) * jnp.where(place < HALF, -1.0, 1.0)
        weight[here, :] = jnp.where(alive, jnp.where(bins == 0, 1.0, 2.0) / period, 0.0) + extra
        return carry

    lax.fori_loop(0, n, phase, 0)

    def transform(r):
        sample = samples[r] * live[:, :step_count]
        for c in range(2):
            value = lax.dot_general(
                forward[c], sample, (((1,), (1,)), ((), ())),
                preferred_element_type=jnp.float32,
            )
            for tile in range(lane_tiles):
                part = value[:, tile * LANES:min(slots, (tile + 1) * LANES)]
                if part.shape[1] < LANES:
                    part = jnp.concatenate(
                        [part, jnp.zeros((part.shape[0], LANES - part.shape[1]), part.dtype)], axis=1
                    )
                spectra[tile, pl.ds(c * rows + r, part.shape[0], stride=per_bin), :] = part

    def transforms(low, high):
        lax.fori_loop(low, high, lambda r, carry: (transform(r), carry)[1], 0)

    def z_row(arrival, d, k):
        return (arrival * 2 + d) * m + k

    def aside_of(parts):
        spot = lax.broadcasted_iota(jnp.int32, (per_bin, LANES), 1)
        lines = []
        for i in range(group - 1):
            line = jnp.zeros((per_bin, LANES), jnp.float32)
            for tile, part in enumerate(parts):
                low, high = max(kept, tile * LANES), min(slots, (tile + 1) * LANES)
                if low < high:
                    turned = pltpu.roll(part[i * per_bin:(i + 1) * per_bin], (i * moved - kept + tile * LANES) % LANES, 1)
                    at = i * moved - kept
                    line = jnp.where((spot >= at + low) & (spot < at + high), turned, line)
            lines.append(line)
        return jnp.concatenate(lines, axis=0)[:, :kept].astype(jnp.bfloat16)

    def contract(arrival, piece):
        d, h = piece
        origin = origin_of(d, arrival)
        noisy = spread[...]
        for k in range(*plan.spans[h]):
            chunk, low, high = plan.parts[d][k]
            row = plan.row(d, k)
            height = plan.height(plan.parts[d][k])
            weights = held[d, origin, row:row + height]
            first = pl.multiple_of((origin * chunks + chunk) * (group * per_bin), group * per_bin)
            parts = [spectra[tile, pl.ds(first, group * per_bin), :] for tile in range(lane_tiles)]
            spec = jnp.concatenate(parts, axis=1)[:, :slots].astype(jnp.bfloat16)
            filled = weights
            if plan.packed(chunk):
                spec = spec[:, :kept]
            elif high - low < slots:
                filled = jnp.concatenate(
                    ([jnp.zeros((low, LANES), jnp.bfloat16)] if low else []) + [weights]
                    + ([jnp.zeros((slots - high, LANES), jnp.bfloat16)] if high < slots else []), axis=0
                )
            product = jnp.dot(spec, filled, preferred_element_type=jnp.float32)
            picked = [product[c * rows:(c + 1) * rows] for c in range(2)]
            for i in range(1, group):
                for c in range(2):
                    at = i * per_bin + c * rows
                    picked[c] = jnp.where(which == i, product[at:at + rows], picked[c])
            if plan.packed(chunk):
                beside = jnp.dot(aside_of(parts), weights, preferred_element_type=jnp.float32)
                for i in range(group - 1):
                    for c in range(2):
                        at = i * per_bin + c * rows
                        back = pltpu.roll(beside[at:at + rows], LANES - (group - 1 - i) * sites, 1)
                        picked[c] += jnp.where(which == i, back, 0.0)
            value = picked[0] + sign * pltpu.roll(picked[1], HALF, 1)
            at = z_row(arrival, d, k)
            z_own[pl.ds(pl.multiple_of(at * rows, rows), rows), :] = value
            z_send[at] = value.astype(jnp.bfloat16)
            wide = weights.astype(jnp.float32)
            known = facts_packed[...] if plan.packed(chunk) else facts[0, low:high]
            power = (wide * wide * known).reshape(height // 8, 8, LANES).sum(axis=0)
            noisy += power * weight[pl.ds(arrival * 2 * pad + d * pad + k, 1), :]
        spread[...] = noisy

    def z_copies(arrival, piece):
        d, h = piece
        low, high = plan.spans[h]
        part = pl.ds(z_row(arrival, d, low), high - low)
        return [
            pltpu.make_async_remote_copy(
                src_ref=z_send.at[part], dst_ref=z_recv.at[p - 1, part],
                send_sem=z_send_sem.at[0], recv_sem=z_recv_sem.at[arrival],
                device_id={"sens": lax.rem(me_s + p, sens_size)}, device_id_type=MESH,
            )
            for p in range(1, sens_size)
        ]

    def send_z(arrival, piece):
        for copy in z_copies(arrival, piece):
            copy.start()

    def receive(step, piece, last=False):
        ring_copy(step, piece, True).wait_recv()
        if not last:
            ring_copy(step + 1, piece, False).start()

    together = LANES // SEAT
    seat_of = lax.broadcasted_iota(jnp.int32, (pad, LANES), 1) // SEAT

    def finish(arrival):
        landed = z_recv.at[:, pl.ds(z_row(arrival, 0, 0), 2 * m)]
        pltpu.make_async_copy(landed, landed, z_recv_sem.at[arrival]).wait()
        for d in range(2):
            for k in range(m):
                at = z_row(arrival, d, k)
                value = z_own[pl.ds(pl.multiple_of(at * rows, rows), rows), :]
                for p in range(1, sens_size):
                    value += z_recv[p - 1, at].astype(jnp.float32)
                near = pl.ds(arrival * 2 * pad + d * pad + k, 1)
                turned_z[d, k * rows:(k + 1) * rows] = (
                    value * cosine[near, :] + pltpu.roll(value, HALF, 1) * sine[near, :]
                )
        for d in range(2):
            for base in range(0, rows, together):
                mine = [turned_z[d, pl.ds(base + j, pad, stride=rows), :] for j in range(together)]
                for c in range(2):
                    for i in range(group):
                        start = c * HALF + i * sites
                        value = None
                        for j in range(together):
                            moved = pltpu.roll(mine[j], (j * SEAT - start) % LANES, 1)
                            value = moved if value is None else jnp.where(seat_of == j, moved, value)
                        low = ((c * group + i) * 2 + d) * pad
                        gathered[low:low + pad, base * SEAT:(base + together) * SEAT] = value.astype(jnp.bfloat16)
        origins = [origin_of(d, arrival) for d in range(2)]
        table = jnp.concatenate(
            [
                inverse[origins[d], at * pad:(at + 1) * pad]
                for at, d in ((2 * ci + d, d) for ci in range(2 * group) for d in range(2))
            ], axis=0
        )
        return lax.dot_general(
            gathered[...], table, (((0,), (0,)), ((), ())), preferred_element_type=jnp.float32
        )

    def finished(low, high):
        def one(arrival, carry):
            total[...] += finish(arrival)
            return carry

        lax.fori_loop(low, high, one, 0)

    for load in loads[3:5]:
        load.wait()
    turns = 2 * halves - 1
    early = rows * 5 // 16
    shares = [early + (rows - early) * turn // turns for turn in range(turns + 1)]
    transforms(0, early)

    def contracts(low, high, piece):
        lax.fori_loop(low, high, lambda arrival, carry: (contract(arrival, piece), carry)[1], 0)

    for step in range(2):
        for h in range(halves):
            for d in range(2):
                receive(step, (d, h))
            at = halves * step + h
            if at < turns:
                transforms(shares[at], shares[at + 1])
    loads[5].wait()
    for piece in pieces:
        contracts(0, 2, piece)
        for arrival in range(2):
            send_z(arrival, piece)

    def middle(step, carry):
        for h in range(halves):
            for d in range(2):
                receive(step, (d, h))
            if h == 0:
                for piece in pieces:
                    contract(step, piece)
                    send_z(step, piece)
            if h == halves - 1:
                finished(step - 2, step - 1)
        return carry

    lax.fori_loop(2, n - 2, middle, 0)
    for piece in pieces:
        contract(n - 2, piece)
        send_z(n - 2, piece)
    finished(n - 4, n - 3)
    for h in range(halves):
        for d in range(2):
            receive(n - 2, (d, h), True)
            contract(n - 1, (d, h))
            send_z(n - 1, (d, h))
        if h == 0:
            finished(n - 3, n - 2)
    spread_send[...] = spread[...]
    spread_copies = [
        pltpu.make_async_remote_copy(
            src_ref=spread_send, dst_ref=spread_recv.at[p - 1],
            send_sem=s_send_sem.at[0], recv_sem=s_recv_sem.at[0],
            device_id={"sens": lax.rem(me_s + p, sens_size)}, device_id_type=MESH,
        )
        for p in range(1, sens_size)
    ]
    for copy in spread_copies:
        copy.start()
    for d in range(2):
        gone = held.at[d, pl.ds(0, n - 1), pl.ds(0, plan.rows[d])]
        pltpu.make_async_copy(gone, gone, ring_send.at[d]).wait()
    finished(n - 2, n - 1)
    result = total[...] + finish(n - 1)
    for tile in range(staged.shape[0]):
        low, high = tile * LANES, min((tile + 1) * LANES, step_count)
        for r in range(rows):
            staged[tile, pl.ds(r, sites, stride=rows), :high - low] = result[r * SEAT:r * SEAT + sites, low:high]
        for q in range(sites):
            out[q, :, low:high] = staged[tile, q * rows:(q + 1) * rows, :high - low].astype(jnp.bfloat16)
    pltpu.make_async_copy(spread_recv, spread_recv, s_send_sem.at[0]).wait()
    pltpu.make_async_copy(spread_recv, spread_recv, s_recv_sem.at[0]).wait()
    summed = spread[...]
    for p in range(1, sens_size):
        summed += spread_recv[p - 1]
    summed = jnp.broadcast_to(jnp.sum(summed, axis=0, keepdims=True), summed.shape)
    summed = summed + pltpu.roll(summed, HALF, 1)
    folded = summed
    for i in range(1, group):
        folded += pltpu.roll(summed, LANES - i * sites, 1)
    spread_out[...] = folded
    pltpu.make_async_copy(z_recv, z_recv, z_send_sem.at[0]).wait()


def on_device(freq_size, sens_size, samples, response_tiles, slot_sensor, sensor_noise, advance_offset):
    bins_dev, _, slots, sites = response_tiles.shape
    rows, _, step_count = samples.shape
    peers = sens_size - 1
    plan = Plan(bins_dev, slots, sites)
    group, chunks, m, pad = plan.group, plan.chunks, plan.m, plan.pad
    forward, inverse = make_tables(freq_size, plan, step_count)
    tiles = response_tiles.transpose(0, 3, 1, 2)
    lane_tiles = -(-slots // LANES)
    count = len(plan.pieces)
    wide = -(-step_count // LANES) * LANES
    vmem = pl.BlockSpec(memory_space=pltpu.VMEM)
    anywhere = pl.BlockSpec(memory_space=pl.ANY)
    operands = (
        tiles, samples, jnp.asarray(forward, jnp.bfloat16), jnp.asarray(inverse, jnp.bfloat16),
        slot_sensor, sensor_noise, advance_offset,
    )
    outlook, spread = pl.pallas_call(
        functools.partial(kernel, freq_size, sens_size, plan),
        out_shape=(
            jax.ShapeDtypeStruct((sites, rows, step_count), jnp.bfloat16),
            jax.ShapeDtypeStruct((8, LANES), jnp.float32),
        ),
        in_specs=[anywhere] * 7,
        out_specs=(vmem, vmem),
        scratch_shapes=[
            pltpu.VMEM(tiles.shape, jnp.bfloat16),
            pltpu.VMEM(samples.shape, jnp.bfloat16),
            pltpu.VMEM(forward.shape, jnp.bfloat16),
            pltpu.VMEM(inverse.shape, jnp.bfloat16),
            pltpu.SMEM(slot_sensor.shape, jnp.int32),
            pltpu.SMEM(sensor_noise.shape, jnp.float32),
            pltpu.SMEM(advance_offset.shape, jnp.int32),
            pltpu.SemaphoreType.DMA((6,)),
            pltpu.SemaphoreType.DMA((count,)),
            pltpu.VMEM((2, slots, LANES), jnp.float32),
            pltpu.VMEM((plan.kept, LANES), jnp.float32),
            pltpu.VMEM((slots, wide), jnp.bfloat16),
            pltpu.VMEM((freq_size * 2 * pad, LANES), jnp.float32),
            pltpu.VMEM((freq_size * 2 * pad, LANES), jnp.float32),
            pltpu.VMEM((freq_size * 2 * pad, LANES), jnp.float32),
            pltpu.VMEM((2, freq_size, plan.held_rows, LANES), jnp.bfloat16),
            pltpu.VMEM((lane_tiles, freq_size * chunks * group * 2 * rows, LANES), jnp.float32),
            pltpu.VMEM((freq_size * 2 * m * rows, LANES), jnp.float32),
            pltpu.VMEM((freq_size * 2 * m, rows, LANES), jnp.bfloat16),
            pltpu.VMEM((peers, freq_size * 2 * m, rows, LANES), jnp.bfloat16),
            pltpu.VMEM((2, pad * rows, LANES), jnp.float32),
            pltpu.VMEM((4 * group * pad, rows * SEAT), jnp.bfloat16),
            pltpu.VMEM((rows * SEAT, step_count), jnp.float32),
            pltpu.VMEM((wide // LANES, sites * rows, LANES), jnp.float32),
            pltpu.VMEM((8, LANES), jnp.float32),
            pltpu.VMEM((8, LANES), jnp.float32),
            pltpu.VMEM((peers, 8, LANES), jnp.float32),
            pltpu.SemaphoreType.DMA((2,)),
            pltpu.SemaphoreType.DMA((count, freq_size - 1)),
            pltpu.SemaphoreType.DMA((1,)),
            pltpu.SemaphoreType.DMA((freq_size,)),
            pltpu.SemaphoreType.DMA((1,)),
            pltpu.SemaphoreType.DMA((1,)),
        ],
        compiler_params=pltpu.CompilerParams(
            collective_id=0, has_side_effects=True, vmem_limit_bytes=50 * 1024 * 1024
        ),
    )(*(pltpu.with_memory_space_constraint(array, pltpu.HBM) for array in operands))
    noise_spread = spread[0, :sites]
    return (outlook.transpose(1, 0, 2), noise_spread)


def solution(mesh):
    placed = (P("freq", "sens", None), P("freq", None, "sens", None), P("sens"), P(), P())
    return jax.shard_map(
        functools.partial(on_device, mesh.shape["freq"], mesh.shape["sens"]),
        mesh=mesh,
        in_specs=placed,
        out_specs=(P("freq", None, None), P()),
        check_vma=False,
    )
```

```python
import functools
import math

import jax
import jax.numpy as jnp
import numpy as np
from jax import lax
from jax.experimental import pallas as pl
from jax.experimental.pallas import tpu as pltpu
from jax.sharding import PartitionSpec as P

MESH = pl.DeviceIdType.MESH
HALF = 64
LANES = 128
SEAT = 32


class Plan:
    def __init__(self, bins_dev, slots, sites):
        self.bins_dev, self.slots, self.sites = bins_dev, slots, sites
        self.group = HALF // sites
        self.chunks = -(-bins_dev // self.group)
        full = self.chunks // 2
        last = self.chunks - 1
        loose = self.group == 3 and bins_dev - last * 3 == 2 and last > 0
        self.moved = slots // 24 * 8 if loose and slots - slots // 24 * 8 <= LANES else 0
        self.kept = slots - self.moved
        cut = (self.kept + 16) // 32 * 16
        plus = [(c, 0, slots) for c in range(full)]
        minus = [(c, 0, slots) for c in range(self.chunks - full, self.chunks)]
        if self.chunks % 2:
            plus.append((full, 0, cut))
            minus.append((full, cut, slots))
        self.parts = (plus, minus)
        self.m = len(plus)
        self.pad = -(-self.m // 16) * 16
        self.rows = [sum(map(self.height, part)) for part in self.parts]
        self.held_rows = -(-max(self.rows) // 16) * 16
        ends = sorted({0, -(-self.m * 3 // 10), self.m - self.m // 5, self.m})
        self.halves = halves = len(ends) - 1
        self.spans = list(zip(ends[:-1], ends[1:]))
        self.pieces = [(d, h) for h in range(halves) for d in range(2)]

    def size(self, chunk):
        return min(self.group, self.bins_dev - chunk * self.group)

    def packed(self, chunk):
        return self.moved > 0 and chunk == self.chunks - 1

    def height(self, entry):
        chunk, low, high = entry
        return self.kept if self.packed(chunk) else high - low

    def row(self, d, k):
        return sum(map(self.height, self.parts[d][:k]))


def make_tables(freq_size, plan, step_count):
    bins_dev, group, chunks = plan.bins_dev, plan.group, plan.chunks
    period = 2 * freq_size * bins_dev
    slot = np.arange(freq_size * chunks * group)
    block, inside = slot // (chunks * group), slot % (chunks * group)
    live = (inside < bins_dev).astype(np.float64)
    bins = np.where(inside < bins_dev, block * bins_dev + inside, 0)
    turns = bins[:, None] * np.arange(step_count)[None, :] % period
    angle = turns * (2.0 * math.pi / period)
    forward = np.stack([np.cos(angle), -np.sin(angle)]) * live[None, :, None]
    inverse = np.zeros((freq_size, 2, group, 2, plan.pad, step_count))
    weight = (np.where(bins == 0, 1.0, 2.0) / period).reshape(freq_size, chunks, group)
    table = forward.reshape(2, freq_size, chunks, group, step_count) * weight[None, ..., None]
    for d in range(2):
        for k, (chunk, _, _) in enumerate(plan.parts[d]):
            inverse[:, :, :, d, k] = table[:, :, chunk].transpose(1, 0, 2, 3)
    return forward, inverse.reshape(freq_size, 4 * group * plan.pad, step_count)


def kernel(
    freq_size, sens_size, plan,
    tiles_in, samples_in, forward_in, inverse_in, slots_in, noise_in, offsets_in,
    out, spread_out,
    raw, samples, forward, inverse, ids, noise, offsets, load_sem, tile_sem,
    facts, facts_packed, live, cosine, sine, weight,
    held, spectra, z_own, z_send, z_recv, turned_z, gathered, total, staged, spread, spread_send, spread_recv,
    ring_send, ring_recv, z_send_sem, z_recv_sem, s_send_sem, s_recv_sem,
):
    rows, slots, step_count = samples.shape
    n, group, chunks, sites, m, pad = freq_size, plan.group, plan.chunks, plan.sites, plan.m, plan.pad
    bins_dev, kept, moved = plan.bins_dev, plan.kept, plan.moved
    per_bin = 2 * rows
    lane_tiles = spectra.shape[0]
    period = 2 * n * bins_dev
    pieces, halves = plan.pieces, plan.halves
    me_f = lax.axis_index("freq")
    me_s = lax.axis_index("sens")

    def position_of(index):
        odd, pair = lax.rem(index, 2), index // 2
        return pair * (1 - odd) + (n - 1 - pair) * odd

    def index_of(position):
        high = position // (n // 2)
        return 2 * position * (1 - high) + (2 * (n - 1 - position) + 1) * high

    me_p = position_of(me_f)

    def along(step):
        return index_of(lax.rem(me_p + step + 2 * n, n))

    def origin_of(d, arrival):
        return along(arrival if d else -arrival)

    tile_loads = []
    for at, (d, h) in enumerate(pieces):
        needed = [
            chunk for chunk, low, high in plan.parts[d][slice(*plan.spans[h])]
            if d == 0 or high - low == slots
        ]
        if needed:
            low = needed[0] * group
            span = pl.ds(low, min((needed[-1] + 1) * group, bins_dev) - low)
            tile_loads.append([pltpu.make_async_copy(tiles_in.at[span], raw.at[span], tile_sem.at[at])])
        else:
            tile_loads.append([])
    loads = [
        pltpu.make_async_copy(source, target, load_sem.at[at])
        for at, (source, target) in enumerate((
            (slots_in, ids), (noise_in, noise), (offsets_in, offsets),
            (forward_in, forward), (samples_in, samples), (inverse_in, inverse),
        ))
    ]
    for load in sum(tile_loads, []) + loads:
        load.start()

    right, left = along(1), along(-1)
    barrier = pltpu.get_barrier_semaphore()
    for neighbour in (left, right):
        pl.semaphore_signal(barrier, inc=1, device_id={"freq": neighbour}, device_id_type=MESH)
    for d in range(1, sens_size):
        peer = lax.rem(me_s + d, sens_size)
        pl.semaphore_signal(barrier, inc=1, device_id={"sens": peer}, device_id_type=MESH)

    def ring_copy(step, piece, received):
        d, h = piece
        low, high = (plan.row(d, k) for k in plan.spans[h])
        origin = origin_of(d, step + (1 if received else 0))
        block = held.at[d, origin, pl.ds(low, high - low)]
        at = 2 * h + d
        return pltpu.make_async_remote_copy(
            src_ref=block, dst_ref=block,
            send_sem=ring_send.at[d], recv_sem=ring_recv.at[at, step],
            device_id={"freq": left if d else right}, device_id_type=MESH,
        )

    line = lax.broadcasted_iota(jnp.int32, (group * sites * 2, LANES), 0)
    spot = lax.broadcasted_iota(jnp.int32, (group * sites * 2, LANES), 1)
    sorter = (spot == lax.rem(line, 2) * HALF + line // 2).astype(jnp.float32).astype(jnp.bfloat16)

    def sort_tiles(d, h):
        for k in range(*plan.spans[h]):
            chunk, low, high = plan.parts[d][k]
            whole = (low, high) == (0, slots)
            if d and not whole:
                continue
            size = plan.size(chunk)
            block = raw[chunk * group:chunk * group + size].reshape(size * sites * 2, slots)
            turned = lax.dot_general(
                block, sorter[:size * sites * 2], (((0,), (0,)), ((), ())),
                preferred_element_type=jnp.float32,
            ).astype(jnp.bfloat16)
            at = plan.row(d, k)
            if plan.packed(chunk):
                aside = []
                for i in range(size):
                    one = raw[chunk * group + i].reshape(sites * 2, slots)
                    aside.append(lax.dot_general(
                        one, sorter[size * sites * 2:], (((0,), (0,)), ((), ())),
                        preferred_element_type=jnp.float32,
                    )[kept:])
                aside.append(jnp.zeros((kept - size * moved, LANES), jnp.float32))
                both = turned[:kept].astype(jnp.float32) + jnp.concatenate(aside, axis=0)
                held[d, me_f, at:at + kept] = both.astype(jnp.bfloat16)
                continue
            held[d, me_f, at:at + high - low] = turned[low:high]
            if not whole:
                at = plan.row(1, m - 1)
                held[1, me_f, at:at + slots - high] = turned[high:]

    for at, piece in enumerate(pieces):
        for load in tile_loads[at]:
            load.wait()
        sort_tiles(*piece)
        if at == 0:
            pl.semaphore_wait(barrier, 2 + sens_size - 1)
        ring_copy(0, piece, False).start()

    for load in loads[:3]:
        load.wait()

    def fact(s, carry):
        sensor = ids[s]
        there = (sensor >= 0).astype(jnp.float32)
        facts[0, pl.ds(s, 1), :] = jnp.full((1, LANES), noise[jnp.maximum(sensor, 0)] * there)
        facts[1, pl.ds(s, 1), :] = jnp.full((1, LANES), there)
        return carry

    lax.fori_loop(0, slots, fact, 0, unroll=8)
    if moved:
        aside = [facts[0, kept:]] * (group - 1) + [jnp.zeros((kept - (group - 1) * moved, LANES), jnp.float32)]
        spare = lax.broadcasted_iota(jnp.int32, (kept, LANES), 1) % HALF // sites == group - 1
        facts_packed[...] = jnp.where(spare, jnp.concatenate(aside, axis=0), facts[0, :kept])
    there = facts[1].astype(jnp.bfloat16)
    live[...] = jnp.concatenate([there] * (live.shape[1] // LANES), axis=1)
    spread[...] = jnp.zeros_like(spread)
    turned_z[...] = jnp.zeros_like(turned_z)
    total[...] = jnp.zeros_like(total)

    lane = lax.broadcasted_iota(jnp.int32, (rows, LANES), 1)
    which = (lane % HALF) // sites
    sign = jnp.where(lane < HALF, -1.0, 1.0).astype(jnp.float32)

    place = lax.broadcasted_iota(jnp.int32, (2 * pad, LANES), 1)
    seat = lax.broadcasted_iota(jnp.int32, (2 * pad, LANES), 0)
    inside = place % HALF
    lead = jnp.zeros((2 * pad, LANES), jnp.float32)
    for q in range(sites):
        lead = jnp.where(inside % sites == q, offsets[q].astype(jnp.float32), lead)
    side = seat // pad
    chunk_of = jnp.zeros_like(seat)
    for d in range(2):
        for k in range(m):
            chunk_of = jnp.where(seat == d * pad + k, plan.parts[d][k][0], chunk_of)
    within = chunk_of * group + inside // sites
    alive = (within < bins_dev) & (inside < group * sites) & (seat % pad < m)
    turning = 2.0 * math.pi / period
    seats = [d * pad + k for d in range(2) for k in range(m) if plan.packed(plan.parts[d][k][0])]
    extra = jnp.zeros((2 * pad, LANES), jnp.float32)
    for row in seats:
        extra = jnp.where((seat == row) & (inside // sites == group - 1), 2.0 / period, extra)

    def phase(arrival, carry):
        block = jnp.where(side == 0, origin_of(0, arrival), origin_of(1, arrival))
        bins = block * bins_dev + within
        ahead = bins.astype(jnp.float32) * lead
        angle = (ahead - period * jnp.floor(ahead / period)) * turning
        here = pl.ds(pl.multiple_of(arrival * 2 * pad, 2 * pad), 2 * pad)
        cosine[here, :] = jnp.cos(angle)
        sine[here, :] = jnp.sin(angle) * jnp.where(place < HALF, -1.0, 1.0)
        weight[here, :] = jnp.where(alive, jnp.where(bins == 0, 1.0, 2.0) / period, 0.0) + extra
        return carry

    lax.fori_loop(0, n, phase, 0)

    def transform(r):
        sample = samples[r] * live[:, :step_count]
        for c in range(2):
            value = lax.dot_general(
                forward[c], sample, (((1,), (1,)), ((), ())),
                preferred_element_type=jnp.float32,
            )
            for tile in range(lane_tiles):
                part = value[:, tile * LANES:min(slots, (tile + 1) * LANES)]
                if part.shape[1] < LANES:
                    part = jnp.concatenate(
                        [part, jnp.zeros((part.shape[0], LANES - part.shape[1]), part.dtype)], axis=1
                    )
                spectra[tile, pl.ds(c * rows + r, part.shape[0], stride=per_bin), :] = part

    def transforms(low, high):
        lax.fori_loop(low, high, lambda r, carry: (transform(r), carry)[1], 0)

    def z_row(arrival, d, k):
        return (arrival * 2 + d) * m + k

    def aside_of(parts):
        spot = lax.broadcasted_iota(jnp.int32, (per_bin, LANES), 1)
        lines = []
        for i in range(group - 1):
            line = jnp.zeros((per_bin, LANES), jnp.float32)
            for tile, part in enumerate(parts):
                low, high = max(kept, tile * LANES), min(slots, (tile + 1) * LANES)
                if low < high:
                    turned = pltpu.roll(part[i * per_bin:(i + 1) * per_bin], (i * moved - kept + tile * LANES) % LANES, 1)
                    at = i * moved - kept
                    line = jnp.where((spot >= at + low) & (spot < at + high), turned, line)
            lines.append(line)
        return jnp.concatenate(lines, axis=0)[:, :kept].astype(jnp.bfloat16)

    def contract(arrival, piece):
        d, h = piece
        origin = origin_of(d, arrival)
        noisy = spread[...]
        for k in range(*plan.spans[h]):
            chunk, low, high = plan.parts[d][k]
            row = plan.row(d, k)
            height = plan.height(plan.parts[d][k])
            weights = held[d, origin, row:row + height]
            first = pl.multiple_of((origin * chunks + chunk) * (group * per_bin), group * per_bin)
            parts = [spectra[tile, pl.ds(first, group * per_bin), :] for tile in range(lane_tiles)]
            spec = jnp.concatenate(parts, axis=1)[:, :slots].astype(jnp.bfloat16)
            filled = weights
            if plan.packed(chunk):
                spec = spec[:, :kept]
            elif high - low < slots:
                filled = jnp.concatenate(
                    ([jnp.zeros((low, LANES), jnp.bfloat16)] if low else []) + [weights]
                    + ([jnp.zeros((slots - high, LANES), jnp.bfloat16)] if high < slots else []), axis=0
                )
            product = jnp.dot(spec, filled, preferred_element_type=jnp.float32)
            picked = [product[c * rows:(c + 1) * rows] for c in range(2)]
            for i in range(1, group):
                for c in range(2):
                    at = i * per_bin + c * rows
                    picked[c] = jnp.where(which == i, product[at:at + rows], picked[c])
            if plan.packed(chunk):
                beside = jnp.dot(aside_of(parts), weights, preferred_element_type=jnp.float32)
                for i in range(group - 1):
                    for c in range(2):
                        at = i * per_bin + c * rows
                        back = pltpu.roll(beside[at:at + rows], LANES - (group - 1 - i) * sites, 1)
                        picked[c] += jnp.where(which == i, back, 0.0)
            value = picked[0] + sign * pltpu.roll(picked[1], HALF, 1)
            at = z_row(arrival, d, k)
            z_own[pl.ds(pl.multiple_of(at * rows, rows), rows), :] = value
            z_send[arrival, d, k] = value.astype(jnp.bfloat16)
            wide = weights.astype(jnp.float32)
            known = facts_packed[...] if plan.packed(chunk) else facts[0, low:high]
            power = (wide * wide * known).reshape(height // 8, 8, LANES).sum(axis=0)
            noisy += power * weight[pl.ds(arrival * 2 * pad + d * pad + k, 1), :]
        spread[...] = noisy

    def z_copies(arrival, piece, last):
        d, h = piece
        low, high = plan.spans[h]
        part = pl.ds(low, high - low)
        return [
            pltpu.make_async_remote_copy(
                src_ref=z_send.at[arrival, d, part], dst_ref=z_recv.at[p - 1, arrival, d, part],
                send_sem=z_send_sem.at[0], recv_sem=z_recv_sem.at[n if last else arrival],
                device_id={"sens": lax.rem(me_s + p, sens_size)}, device_id_type=MESH,
            )
            for p in range(1, sens_size)
        ]

    def send_z(arrival, piece, last=False):
        for copy in z_copies(arrival, piece, last):
            copy.start()

    def receive(step, piece, last=False):
        ring_copy(step, piece, True).wait_recv()
        if not last:
            ring_copy(step + 1, piece, False).start()

    together = LANES // SEAT
    seat_of = lax.broadcasted_iota(jnp.int32, (pad, LANES), 1) // SEAT

    def combine(arrival, low, high):
        for d in range(2):
            for k in range(low, high):
                at = z_row(arrival, d, k)
                value = z_own[pl.ds(pl.multiple_of(at * rows, rows), rows), :]
                for p in range(1, sens_size):
                    value += z_recv[p - 1, arrival, d, k].astype(jnp.float32)
                near = pl.ds(arrival * 2 * pad + d * pad + k, 1)
                turned_z[d, k * rows:(k + 1) * rows] = (
                    value * cosine[near, :] + pltpu.roll(value, HALF, 1) * sine[near, :]
                )

    def table_of(arrival):
        origins = [origin_of(d, arrival) for d in range(2)]
        return jnp.concatenate(
            [
                inverse[origins[d], at * pad:(at + 1) * pad]
                for at, d in ((2 * ci + d, d) for ci in range(2 * group) for d in range(2))
            ], axis=0
        )

    def gather(base):
        for d in range(2):
            mine = [turned_z[d, pl.ds(base + j, pad, stride=rows), :] for j in range(together)]
            for c in range(2):
                for i in range(group):
                    start = c * HALF + i * sites
                    value = None
                    for j in range(together):
                        moved_to = pltpu.roll(mine[j], (j * SEAT - start) % LANES, 1)
                        value = moved_to if value is None else jnp.where(seat_of == j, moved_to, value)
                    low = ((c * group + i) * 2 + d) * pad
                    gathered[low:low + pad, base * SEAT:(base + together) * SEAT] = value.astype(jnp.bfloat16)

    def times(block, table):
        return lax.dot_general(block, table, (((0,), (0,)), ((), ())), preferred_element_type=jnp.float32)

    def invert(arrival):
        for base in range(0, rows, together):
            gather(base)
        return times(gathered[...], table_of(arrival))

    def finished(low, high):
        def one(arrival, carry):
            landed = z_recv.at[:, arrival]
            pltpu.make_async_copy(landed, landed, z_recv_sem.at[arrival]).wait()
            combine(arrival, 0, m)
            total[...] += invert(arrival)
            return carry

        lax.fori_loop(low, high, one, 0)

    for load in loads[3:5]:
        load.wait()
    turns = 2 * halves - 1
    early = rows * 5 // 16
    shares = [early + (rows - early) * turn // turns for turn in range(turns + 1)]
    transforms(0, early)

    def contracts(low, high, piece):
        lax.fori_loop(low, high, lambda arrival, carry: (contract(arrival, piece), carry)[1], 0)

    for step in range(2):
        for h in range(halves):
            for d in range(2):
                receive(step, (d, h))
            at = halves * step + h
            if at < turns:
                transforms(shares[at], shares[at + 1])
    loads[5].wait()
    for piece in pieces:
        contracts(0, 2, piece)
        for arrival in range(2):
            send_z(arrival, piece)

    def middle(step, carry):
        for h in range(halves):
            for d in range(2):
                receive(step, (d, h))
            if h == 0:
                for piece in pieces:
                    contract(step, piece)
                    send_z(step, piece)
            if h == halves - 1:
                finished(step - 2, step - 1)
        return carry

    lax.fori_loop(2, n - 2, middle, 0)
    for piece in pieces:
        contract(n - 2, piece)
        send_z(n - 2, piece)
    finished(n - 4, n - 3)
    spread_copies = [
        pltpu.make_async_remote_copy(
            src_ref=spread_send, dst_ref=spread_recv.at[p - 1],
            send_sem=s_send_sem.at[0], recv_sem=s_recv_sem.at[0],
            device_id={"sens": lax.rem(me_s + p, sens_size)}, device_id_type=MESH,
        )
        for p in range(1, sens_size)
    ]
    for h in range(halves):
        for d in range(2):
            receive(n - 2, (d, h), True)
            contract(n - 1, (d, h))
            if (d, h) == pieces[-1]:
                spread_send[...] = spread[...]
                for copy in spread_copies:
                    copy.start()
            send_z(n - 1, (d, h), h == halves - 1)
        if h == 0:
            finished(n - 3, n - 2)
    for d in range(2):
        gone = held.at[d, pl.ds(0, n - 1), pl.ds(0, plan.rows[d])]
        pltpu.make_async_copy(gone, gone, ring_send.at[d]).wait()
    finished(n - 2, n - 1)
    split = plan.spans[-1][0]
    for low, high, at in ((0, split, n - 1), (split, m, n)):
        if at == n:
            pltpu.make_async_copy(spread_recv, spread_recv, s_send_sem.at[0]).wait()
            pltpu.make_async_copy(spread_recv, spread_recv, s_recv_sem.at[0]).wait()
            summed = spread[...]
            for p in range(1, sens_size):
                summed += spread_recv[p - 1]
            summed = jnp.broadcast_to(jnp.sum(summed, axis=0, keepdims=True), summed.shape)
            summed = summed + pltpu.roll(summed, HALF, 1)
            folded = summed
            for i in range(1, group):
                folded += pltpu.roll(summed, LANES - i * sites, 1)
            spread_out[...] = folded[:1, :sites]
        landed = z_recv.at[:, n - 1, :, pl.ds(low, high - low)]
        pltpu.make_async_copy(landed, landed, z_recv_sem.at[at]).wait()
        combine(n - 1, low, high)
    table = table_of(n - 1)
    for base in range(0, rows, together):
        gather(base)
        span = slice(base * SEAT, (base + together) * SEAT)
        result = total[span] + times(gathered[:, span], table)
        for tile in range(staged.shape[0]):
            low, high = tile * LANES, min((tile + 1) * LANES, step_count)
            for j in range(together):
                staged[tile, pl.ds(base + j, sites, stride=rows), :high - low] = (
                    result[j * SEAT:j * SEAT + sites, low:high]
                )
    for tile in range(staged.shape[0]):
        low, high = tile * LANES, min((tile + 1) * LANES, step_count)
        for q in range(sites):
            out[q, :, low:high] = staged[tile, q * rows:(q + 1) * rows, :high - low].astype(jnp.bfloat16)
    pltpu.make_async_copy(z_recv, z_recv, z_send_sem.at[0]).wait()


def hand_out(outlook_in, spread_in, outlook_out, spread_out, sem):
    copies = [
        pltpu.make_async_copy(source, target, sem.at[at])
        for at, (source, target) in enumerate(((outlook_in, outlook_out), (spread_in, spread_out)))
    ]
    for copy in copies:
        copy.start()
    for copy in copies:
        copy.wait()


def on_device(freq_size, sens_size, samples, response_tiles, slot_sensor, sensor_noise, advance_offset):
    bins_dev, _, slots, sites = response_tiles.shape
    rows, _, step_count = samples.shape
    peers = sens_size - 1
    plan = Plan(bins_dev, slots, sites)
    group, chunks, m, pad = plan.group, plan.chunks, plan.m, plan.pad
    forward, inverse = make_tables(freq_size, plan, step_count)
    tiles = response_tiles.transpose(0, 3, 1, 2)
    lane_tiles = -(-slots // LANES)
    count = len(plan.pieces)
    wide = -(-step_count // LANES) * LANES
    vmem = pl.BlockSpec(memory_space=pltpu.VMEM)
    anywhere = pl.BlockSpec(memory_space=pl.ANY)
    operands = (
        tiles, samples, jnp.asarray(forward, jnp.bfloat16), jnp.asarray(inverse, jnp.bfloat16),
        slot_sensor, sensor_noise, advance_offset,
    )
    outlook, spread = pl.pallas_call(
        functools.partial(kernel, freq_size, sens_size, plan),
        out_shape=(
            jax.ShapeDtypeStruct((sites, rows, step_count), jnp.bfloat16),
            jax.ShapeDtypeStruct((1, sites), jnp.float32),
        ),
        in_specs=[anywhere] * 7,
        out_specs=(vmem, vmem),
        scratch_shapes=[
            pltpu.VMEM(tiles.shape, jnp.bfloat16),
            pltpu.VMEM(samples.shape, jnp.bfloat16),
            pltpu.VMEM(forward.shape, jnp.bfloat16),
            pltpu.VMEM(inverse.shape, jnp.bfloat16),
            pltpu.SMEM(slot_sensor.shape, jnp.int32),
            pltpu.SMEM(sensor_noise.shape, jnp.float32),
            pltpu.SMEM(advance_offset.shape, jnp.int32),
            pltpu.SemaphoreType.DMA((6,)),
            pltpu.SemaphoreType.DMA((count,)),
            pltpu.VMEM((2, slots, LANES), jnp.float32),
            pltpu.VMEM((plan.kept, LANES), jnp.float32),
            pltpu.VMEM((slots, wide), jnp.bfloat16),
            pltpu.VMEM((freq_size * 2 * pad, LANES), jnp.float32),
            pltpu.VMEM((freq_size * 2 * pad, LANES), jnp.float32),
            pltpu.VMEM((freq_size * 2 * pad, LANES), jnp.float32),
            pltpu.VMEM((2, freq_size, plan.held_rows, LANES), jnp.bfloat16),
            pltpu.VMEM((lane_tiles, freq_size * chunks * group * 2 * rows, LANES), jnp.float32),
            pltpu.VMEM((freq_size * 2 * m * rows, LANES), jnp.float32),
            pltpu.VMEM((freq_size, 2, m, rows, LANES), jnp.bfloat16),
            pltpu.VMEM((peers, freq_size, 2, m, rows, LANES), jnp.bfloat16),
            pltpu.VMEM((2, pad * rows, LANES), jnp.float32),
            pltpu.VMEM((4 * group * pad, rows * SEAT), jnp.bfloat16),
            pltpu.VMEM((rows * SEAT, step_count), jnp.float32),
            pltpu.VMEM((wide // LANES, sites * rows, LANES), jnp.float32),
            pltpu.VMEM((8, LANES), jnp.float32),
            pltpu.VMEM((8, LANES), jnp.float32),
            pltpu.VMEM((peers, 8, LANES), jnp.float32),
            pltpu.SemaphoreType.DMA((2,)),
            pltpu.SemaphoreType.DMA((count, freq_size - 1)),
            pltpu.SemaphoreType.DMA((1,)),
            pltpu.SemaphoreType.DMA((freq_size + 1,)),
            pltpu.SemaphoreType.DMA((1,)),
            pltpu.SemaphoreType.DMA((1,)),
        ],
        compiler_params=pltpu.CompilerParams(
            collective_id=0, has_side_effects=True, vmem_limit_bytes=50 * 1024 * 1024
        ),
    )(*(pltpu.with_memory_space_constraint(array, pltpu.HBM) for array in operands))
    outlook, spread = pl.pallas_call(
        hand_out,
        out_shape=(
            jax.ShapeDtypeStruct(outlook.shape, outlook.dtype),
            jax.ShapeDtypeStruct(spread.shape, spread.dtype),
        ),
        in_specs=[anywhere] * 2,
        out_specs=(anywhere, anywhere),
        scratch_shapes=[pltpu.SemaphoreType.DMA((2,))],
        compiler_params=pltpu.CompilerParams(vmem_limit_bytes=1024 * 1024),
    )(outlook, spread)
    return (outlook.transpose(1, 0, 2), spread.reshape(sites))


def solution(mesh):
    placed = (P("freq", "sens", None), P("freq", None, "sens", None), P("sens"), P(), P())
    return jax.shard_map(
        functools.partial(on_device, mesh.shape["freq"], mesh.shape["sens"]),
        mesh=mesh,
        in_specs=placed,
        out_specs=(P("freq", None, None), P()),
        check_vma=False,
    )
```

```python
import functools
import math

import jax
import jax.numpy as jnp
import numpy as np
from jax import lax
from jax.experimental import pallas as pl
from jax.experimental.pallas import tpu as pltpu
from jax.sharding import PartitionSpec as P

MESH = pl.DeviceIdType.MESH
HALF = 64
LANES = 128
SEAT = 32


class Plan:
    def __init__(self, bins_dev, slots, sites):
        self.bins_dev, self.slots, self.sites = bins_dev, slots, sites
        self.group = HALF // sites
        self.chunks = -(-bins_dev // self.group)
        full = self.chunks // 2
        last = self.chunks - 1
        loose = self.group == 3 and bins_dev - last * 3 == 2 and last > 0
        self.moved = slots // 24 * 8 if loose and slots - slots // 24 * 8 <= LANES else 0
        self.kept = slots - self.moved
        cut = (self.kept + 16) // 32 * 16
        plus = [(c, 0, slots) for c in range(full)]
        minus = [(c, 0, slots) for c in range(self.chunks - full, self.chunks)]
        if self.chunks % 2:
            plus.append((full, 0, cut))
            minus.append((full, cut, slots))
        self.parts = (plus, minus)
        self.m = len(plus)
        self.pad = -(-self.m // 16) * 16
        self.rows = [sum(map(self.height, part)) for part in self.parts]
        self.held_rows = -(-max(self.rows) // 16) * 16
        ends = sorted({0, self.m * 6 // 10, self.m})
        self.halves = halves = len(ends) - 1
        self.spans = list(zip(ends[:-1], ends[1:]))
        self.pieces = [(d, h) for h in range(halves) for d in range(2)]

    def size(self, chunk):
        return min(self.group, self.bins_dev - chunk * self.group)

    def packed(self, chunk):
        return self.moved > 0 and chunk == self.chunks - 1

    def height(self, entry):
        chunk, low, high = entry
        return self.kept if self.packed(chunk) else high - low

    def row(self, d, k):
        return sum(map(self.height, self.parts[d][:k]))


def make_tables(freq_size, plan, step_count):
    bins_dev, group, chunks = plan.bins_dev, plan.group, plan.chunks
    period = 2 * freq_size * bins_dev
    slot = np.arange(freq_size * chunks * group)
    block, inside = slot // (chunks * group), slot % (chunks * group)
    live = (inside < bins_dev).astype(np.float64)
    bins = np.where(inside < bins_dev, block * bins_dev + inside, 0)
    turns = bins[:, None] * np.arange(step_count)[None, :] % period
    angle = turns * (2.0 * math.pi / period)
    forward = np.stack([np.cos(angle), -np.sin(angle)]) * live[None, :, None]
    inverse = np.zeros((freq_size, 2, group, 2, plan.pad, step_count))
    weight = (np.where(bins == 0, 1.0, 2.0) / period).reshape(freq_size, chunks, group)
    table = forward.reshape(2, freq_size, chunks, group, step_count) * weight[None, ..., None]
    for d in range(2):
        for k, (chunk, _, _) in enumerate(plan.parts[d]):
            inverse[:, :, :, d, k] = table[:, :, chunk].transpose(1, 0, 2, 3)
    return forward, inverse.reshape(freq_size, 4 * group * plan.pad, step_count)


def kernel(
    freq_size, sens_size, plan,
    tiles_in, samples_in, forward_in, inverse_in, slots_in, noise_in, offsets_in,
    out, spread_out,
    raw, samples, forward, inverse, ids, noise, offsets, load_sem, tile_sem,
    facts, facts_packed, live, cosine, sine, weight,
    held, spectra, z_own, z_send, z_recv, turned_z, gathered, total, staged, spread, spread_send, spread_recv,
    ring_send, ring_recv, z_send_sem, z_recv_sem, s_send_sem, s_recv_sem,
):
    rows, slots, step_count = samples.shape
    n, group, chunks, sites, m, pad = freq_size, plan.group, plan.chunks, plan.sites, plan.m, plan.pad
    bins_dev, kept, moved = plan.bins_dev, plan.kept, plan.moved
    per_bin = 2 * rows
    lane_tiles = spectra.shape[0]
    period = 2 * n * bins_dev
    pieces, halves = plan.pieces, plan.halves
    me_f = lax.axis_index("freq")
    me_s = lax.axis_index("sens")

    def position_of(index):
        odd, pair = lax.rem(index, 2), index // 2
        return pair * (1 - odd) + (n - 1 - pair) * odd

    def index_of(position):
        high = position // (n // 2)
        return 2 * position * (1 - high) + (2 * (n - 1 - position) + 1) * high

    me_p = position_of(me_f)

    def along(step):
        return index_of(lax.rem(me_p + step + 2 * n, n))

    def origin_of(d, arrival):
        return along(arrival if d else -arrival)

    tile_loads = []
    for at, (d, h) in enumerate(pieces):
        needed = [
            chunk for chunk, low, high in plan.parts[d][slice(*plan.spans[h])]
            if d == 0 or high - low == slots
        ]
        if needed:
            low = needed[0] * group
            span = pl.ds(low, min((needed[-1] + 1) * group, bins_dev) - low)
            tile_loads.append([pltpu.make_async_copy(tiles_in.at[span], raw.at[span], tile_sem.at[at])])
        else:
            tile_loads.append([])
    loads = [
        pltpu.make_async_copy(source, target, load_sem.at[at])
        for at, (source, target) in enumerate((
            (slots_in, ids), (noise_in, noise), (offsets_in, offsets),
            (forward_in, forward), (samples_in, samples), (inverse_in, inverse),
        ))
    ]
    for load in sum(tile_loads, []):
        load.start()

    right, left = along(1), along(-1)
    barrier = pltpu.get_barrier_semaphore()
    for neighbour in (left, right):
        pl.semaphore_signal(barrier, inc=1, device_id={"freq": neighbour}, device_id_type=MESH)
    for d in range(1, sens_size):
        peer = lax.rem(me_s + d, sens_size)
        pl.semaphore_signal(barrier, inc=1, device_id={"sens": peer}, device_id_type=MESH)

    def ring_copy(step, piece, received):
        d, h = piece
        low, high = (plan.row(d, k) for k in plan.spans[h])
        origin = origin_of(d, step + (1 if received else 0))
        block = held.at[d, origin, pl.ds(low, high - low)]
        at = 2 * h + d
        return pltpu.make_async_remote_copy(
            src_ref=block, dst_ref=block,
            send_sem=ring_send.at[d], recv_sem=ring_recv.at[at, step],
            device_id={"freq": left if d else right}, device_id_type=MESH,
        )

    line = lax.broadcasted_iota(jnp.int32, (group * sites * 2, LANES), 0)
    spot = lax.broadcasted_iota(jnp.int32, (group * sites * 2, LANES), 1)
    sorter = (spot == lax.rem(line, 2) * HALF + line // 2).astype(jnp.float32).astype(jnp.bfloat16)

    def sort_tiles(d, h):
        for k in range(*plan.spans[h]):
            chunk, low, high = plan.parts[d][k]
            whole = (low, high) == (0, slots)
            if d and not whole:
                continue
            size = plan.size(chunk)
            block = raw[chunk * group:chunk * group + size].reshape(size * sites * 2, slots)
            turned = lax.dot_general(
                block, sorter[:size * sites * 2], (((0,), (0,)), ((), ())),
                preferred_element_type=jnp.float32,
            ).astype(jnp.bfloat16)
            at = plan.row(d, k)
            if plan.packed(chunk):
                aside = []
                for i in range(size):
                    one = raw[chunk * group + i].reshape(sites * 2, slots)
                    aside.append(lax.dot_general(
                        one, sorter[size * sites * 2:], (((0,), (0,)), ((), ())),
                        preferred_element_type=jnp.float32,
                    )[kept:])
                aside.append(jnp.zeros((kept - size * moved, LANES), jnp.float32))
                both = turned[:kept].astype(jnp.float32) + jnp.concatenate(aside, axis=0)
                held[d, me_f, at:at + kept] = both.astype(jnp.bfloat16)
                continue
            held[d, me_f, at:at + high - low] = turned[low:high]
            if not whole:
                at = plan.row(1, m - 1)
                held[1, me_f, at:at + slots - high] = turned[high:]

    for at, piece in enumerate(pieces):
        for load in tile_loads[at]:
            load.wait()
        sort_tiles(*piece)
        if at == 0:
            pl.semaphore_wait(barrier, 2 + sens_size - 1)
        ring_copy(0, piece, False).start()
        if at == 1:
            for load in loads:
                load.start()

    for load in loads[:3]:
        load.wait()

    def fact(s, carry):
        sensor = ids[s]
        there = (sensor >= 0).astype(jnp.float32)
        facts[0, pl.ds(s, 1), :] = jnp.full((1, LANES), noise[jnp.maximum(sensor, 0)] * there)
        facts[1, pl.ds(s, 1), :] = jnp.full((1, LANES), there)
        return carry

    lax.fori_loop(0, slots, fact, 0, unroll=8)
    if moved:
        aside = [facts[0, kept:]] * (group - 1) + [jnp.zeros((kept - (group - 1) * moved, LANES), jnp.float32)]
        spare = lax.broadcasted_iota(jnp.int32, (kept, LANES), 1) % HALF // sites == group - 1
        facts_packed[...] = jnp.where(spare, jnp.concatenate(aside, axis=0), facts[0, :kept])
    there = facts[1].astype(jnp.bfloat16)
    live[...] = jnp.concatenate([there] * (live.shape[1] // LANES), axis=1)
    spread[...] = jnp.zeros_like(spread)
    turned_z[...] = jnp.zeros_like(turned_z)
    total[...] = jnp.zeros_like(total)

    lane = lax.broadcasted_iota(jnp.int32, (rows, LANES), 1)
    which = (lane % HALF) // sites
    sign = jnp.where(lane < HALF, -1.0, 1.0).astype(jnp.float32)

    place = lax.broadcasted_iota(jnp.int32, (2 * pad, LANES), 1)
    seat = lax.broadcasted_iota(jnp.int32, (2 * pad, LANES), 0)
    inside = place % HALF
    lead = jnp.zeros((2 * pad, LANES), jnp.float32)
    for q in range(sites):
        lead = jnp.where(inside % sites == q, offsets[q].astype(jnp.float32), lead)
    side = seat // pad
    chunk_of = jnp.zeros_like(seat)
    for d in range(2):
        for k in range(m):
            chunk_of = jnp.where(seat == d * pad + k, plan.parts[d][k][0], chunk_of)
    within = chunk_of * group + inside // sites
    alive = (within < bins_dev) & (inside < group * sites) & (seat % pad < m)
    turning = 2.0 * math.pi / period
    seats = [d * pad + k for d in range(2) for k in range(m) if plan.packed(plan.parts[d][k][0])]
    extra = jnp.zeros((2 * pad, LANES), jnp.float32)
    for row in seats:
        extra = jnp.where((seat == row) & (inside // sites == group - 1), 2.0 / period, extra)

    def phase(arrival, carry):
        block = jnp.where(side == 0, origin_of(0, arrival), origin_of(1, arrival))
        bins = block * bins_dev + within
        ahead = bins.astype(jnp.float32) * lead
        angle = (ahead - period * jnp.floor(ahead / period)) * turning
        here = pl.ds(pl.multiple_of(arrival * 2 * pad, 2 * pad), 2 * pad)
        cosine[here, :] = jnp.cos(angle)
        sine[here, :] = jnp.sin(angle) * jnp.where(place < HALF, -1.0, 1.0)
        weight[here, :] = jnp.where(alive, jnp.where(bins == 0, 1.0, 2.0) / period, 0.0) + extra
        return carry

    lax.fori_loop(0, n, phase, 0)

    def transform(r):
        sample = samples[r] * live[:, :step_count]
        for c in range(2):
            value = lax.dot_general(
                forward[c], sample, (((1,), (1,)), ((), ())),
                preferred_element_type=jnp.float32,
            )
            for tile in range(lane_tiles):
                part = value[:, tile * LANES:min(slots, (tile + 1) * LANES)]
                if part.shape[1] < LANES:
                    part = jnp.concatenate(
                        [part, jnp.zeros((part.shape[0], LANES - part.shape[1]), part.dtype)], axis=1
                    )
                spectra[tile, pl.ds(c * rows + r, part.shape[0], stride=per_bin), :] = part

    def transforms(low, high):
        lax.fori_loop(low, high, lambda r, carry: (transform(r), carry)[1], 0)

    def z_row(arrival, d, k):
        return (arrival * 2 + d) * m + k

    def aside_of(parts):
        spot = lax.broadcasted_iota(jnp.int32, (per_bin, LANES), 1)
        lines = []
        for i in range(group - 1):
            line = jnp.zeros((per_bin, LANES), jnp.float32)
            for tile, part in enumerate(parts):
                low, high = max(kept, tile * LANES), min(slots, (tile + 1) * LANES)
                if low < high:
                    turned = pltpu.roll(part[i * per_bin:(i + 1) * per_bin], (i * moved - kept + tile * LANES) % LANES, 1)
                    at = i * moved - kept
                    line = jnp.where((spot >= at + low) & (spot < at + high), turned, line)
            lines.append(line)
        return jnp.concatenate(lines, axis=0)[:, :kept].astype(jnp.bfloat16)

    def contract(arrival, piece):
        d, h = piece
        origin = origin_of(d, arrival)
        noisy = spread[...]
        for k in range(*plan.spans[h]):
            chunk, low, high = plan.parts[d][k]
            row = plan.row(d, k)
            height = plan.height(plan.parts[d][k])
            weights = held[d, origin, row:row + height]
            first = pl.multiple_of((origin * chunks + chunk) * (group * per_bin), group * per_bin)
            parts = [spectra[tile, pl.ds(first, group * per_bin), :] for tile in range(lane_tiles)]
            spec = jnp.concatenate(parts, axis=1)[:, :slots].astype(jnp.bfloat16)
            filled = weights
            if plan.packed(chunk):
                spec = spec[:, :kept]
            elif high - low < slots:
                filled = jnp.concatenate(
                    ([jnp.zeros((low, LANES), jnp.bfloat16)] if low else []) + [weights]
                    + ([jnp.zeros((slots - high, LANES), jnp.bfloat16)] if high < slots else []), axis=0
                )
            product = jnp.dot(spec, filled, preferred_element_type=jnp.float32)
            picked = [product[c * rows:(c + 1) * rows] for c in range(2)]
            for i in range(1, group):
                for c in range(2):
                    at = i * per_bin + c * rows
                    picked[c] = jnp.where(which == i, product[at:at + rows], picked[c])
            if plan.packed(chunk):
                beside = jnp.dot(aside_of(parts), weights, preferred_element_type=jnp.float32)
                for i in range(group - 1):
                    for c in range(2):
                        at = i * per_bin + c * rows
                        back = pltpu.roll(beside[at:at + rows], LANES - (group - 1 - i) * sites, 1)
                        picked[c] += jnp.where(which == i, back, 0.0)
            value = picked[0] + sign * pltpu.roll(picked[1], HALF, 1)
            at = z_row(arrival, d, k)
            z_own[pl.ds(pl.multiple_of(at * rows, rows), rows), :] = value
            z_send[arrival, d, k] = value.astype(jnp.bfloat16)
            wide = weights.astype(jnp.float32)
            known = facts_packed[...] if plan.packed(chunk) else facts[0, low:high]
            power = (wide * wide * known).reshape(height // 8, 8, LANES).sum(axis=0)
            noisy += power * weight[pl.ds(arrival * 2 * pad + d * pad + k, 1), :]
        spread[...] = noisy

    def z_copies(arrival, piece, last):
        d, h = piece
        low, high = plan.spans[h]
        part = pl.ds(low, high - low)
        return [
            pltpu.make_async_remote_copy(
                src_ref=z_send.at[arrival, d, part], dst_ref=z_recv.at[p - 1, arrival, d, part],
                send_sem=z_send_sem.at[0], recv_sem=z_recv_sem.at[n if last else arrival],
                device_id={"sens": lax.rem(me_s + p, sens_size)}, device_id_type=MESH,
            )
            for p in range(1, sens_size)
        ]

    def send_z(arrival, piece, last=False):
        for copy in z_copies(arrival, piece, last):
            copy.start()

    def receive(step, piece, last=False):
        ring_copy(step, piece, True).wait_recv()
        if not last:
            ring_copy(step + 1, piece, False).start()

    together = LANES // SEAT
    seat_of = lax.broadcasted_iota(jnp.int32, (pad, LANES), 1) // SEAT

    def combine(arrival, low, high):
        for d in range(2):
            for k in range(low, high):
                at = z_row(arrival, d, k)
                value = z_own[pl.ds(pl.multiple_of(at * rows, rows), rows), :]
                for p in range(1, sens_size):
                    value += z_recv[p - 1, arrival, d, k].astype(jnp.float32)
                near = pl.ds(arrival * 2 * pad + d * pad + k, 1)
                turned_z[d, k * rows:(k + 1) * rows] = (
                    value * cosine[near, :] + pltpu.roll(value, HALF, 1) * sine[near, :]
                )

    def table_of(arrival):
        origins = [origin_of(d, arrival) for d in range(2)]
        return jnp.concatenate(
            [
                inverse[origins[d], at * pad:(at + 1) * pad]
                for at, d in ((2 * ci + d, d) for ci in range(2 * group) for d in range(2))
            ], axis=0
        )

    def gather(base):
        for d in range(2):
            mine = [turned_z[d, pl.ds(base + j, pad, stride=rows), :] for j in range(together)]
            for c in range(2):
                for i in range(group):
                    start = c * HALF + i * sites
                    value = None
                    for j in range(together):
                        moved_to = pltpu.roll(mine[j], (j * SEAT - start) % LANES, 1)
                        value = moved_to if value is None else jnp.where(seat_of == j, moved_to, value)
                    low = ((c * group + i) * 2 + d) * pad
                    gathered[low:low + pad, base * SEAT:(base + together) * SEAT] = value.astype(jnp.bfloat16)

    def times(block, table):
        return lax.dot_general(block, table, (((0,), (0,)), ((), ())), preferred_element_type=jnp.float32)

    def invert(arrival):
        for base in range(0, rows, together):
            gather(base)
        return times(gathered[...], table_of(arrival))

    def finished(low, high):
        def one(arrival, carry):
            landed = z_recv.at[:, arrival]
            pltpu.make_async_copy(landed, landed, z_recv_sem.at[arrival]).wait()
            combine(arrival, 0, m)
            total[...] += invert(arrival)
            return carry

        lax.fori_loop(low, high, one, 0)

    for load in loads[3:5]:
        load.wait()
    turns = 2 * halves - 1
    early = rows * 5 // 16
    shares = [early + (rows - early) * turn // turns for turn in range(turns + 1)]
    transforms(0, early)

    def contracts(low, high, piece):
        lax.fori_loop(low, high, lambda arrival, carry: (contract(arrival, piece), carry)[1], 0)

    for step in range(2):
        for h in range(halves):
            for d in range(2):
                receive(step, (d, h))
            at = halves * step + h
            if at < turns:
                transforms(shares[at], shares[at + 1])
    loads[5].wait()
    for piece in pieces:
        contracts(0, 2, piece)
        for arrival in range(2):
            send_z(arrival, piece)

    def middle(step, carry):
        for h in range(halves):
            for d in range(2):
                receive(step, (d, h))
            if h == 0:
                for piece in pieces:
                    contract(step, piece)
                    send_z(step, piece)
            if h == halves - 1:
                finished(step - 2, step - 1)
        return carry

    lax.fori_loop(2, n - 2, middle, 0)
    for piece in pieces:
        contract(n - 2, piece)
        send_z(n - 2, piece)
    finished(n - 4, n - 3)
    spread_copies = [
        pltpu.make_async_remote_copy(
            src_ref=spread_send, dst_ref=spread_recv.at[p - 1],
            send_sem=s_send_sem.at[0], recv_sem=s_recv_sem.at[0],
            device_id={"sens": lax.rem(me_s + p, sens_size)}, device_id_type=MESH,
        )
        for p in range(1, sens_size)
    ]
    for h in range(halves):
        for d in range(2):
            receive(n - 2, (d, h), True)
            contract(n - 1, (d, h))
            if (d, h) == pieces[-1]:
                spread_send[...] = spread[...]
                for copy in spread_copies:
                    copy.start()
            send_z(n - 1, (d, h), h == halves - 1)
        if h == 0:
            finished(n - 3, n - 2)
    for d in range(2):
        gone = held.at[d, pl.ds(0, n - 1), pl.ds(0, plan.rows[d])]
        pltpu.make_async_copy(gone, gone, ring_send.at[d]).wait()
    finished(n - 2, n - 1)
    split = plan.spans[-1][0]
    for low, high, at in ((0, split, n - 1), (split, m, n)):
        if at == n:
            pltpu.make_async_copy(spread_recv, spread_recv, s_send_sem.at[0]).wait()
            pltpu.make_async_copy(spread_recv, spread_recv, s_recv_sem.at[0]).wait()
            summed = spread[...]
            for p in range(1, sens_size):
                summed += spread_recv[p - 1]
            summed = jnp.broadcast_to(jnp.sum(summed, axis=0, keepdims=True), summed.shape)
            summed = summed + pltpu.roll(summed, HALF, 1)
            folded = summed
            for i in range(1, group):
                folded += pltpu.roll(summed, LANES - i * sites, 1)
            spread_out[...] = folded[:1, :sites]
        landed = z_recv.at[:, n - 1, :, pl.ds(low, high - low)]
        pltpu.make_async_copy(landed, landed, z_recv_sem.at[at]).wait()
        combine(n - 1, low, high)
    table = table_of(n - 1)
    for base in range(0, rows, together):
        gather(base)
        span = slice(base * SEAT, (base + together) * SEAT)
        result = total[span] + times(gathered[:, span], table)
        for tile in range(staged.shape[0]):
            low, high = tile * LANES, min((tile + 1) * LANES, step_count)
            for j in range(together):
                staged[tile, pl.ds(base + j, sites, stride=rows), :high - low] = (
                    result[j * SEAT:j * SEAT + sites, low:high]
                )
    for tile in range(staged.shape[0]):
        low, high = tile * LANES, min((tile + 1) * LANES, step_count)
        for q in range(sites):
            out[q, :, low:high] = staged[tile, q * rows:(q + 1) * rows, :high - low].astype(jnp.bfloat16)
    pltpu.make_async_copy(z_recv, z_recv, z_send_sem.at[0]).wait()


def hand_out(outlook_in, spread_in, outlook_out, spread_out, sem):
    copies = [
        pltpu.make_async_copy(source, target, sem.at[at])
        for at, (source, target) in enumerate(((outlook_in, outlook_out), (spread_in, spread_out)))
    ]
    for copy in copies:
        copy.start()
    for copy in copies:
        copy.wait()


def on_device(freq_size, sens_size, samples, response_tiles, slot_sensor, sensor_noise, advance_offset):
    bins_dev, _, slots, sites = response_tiles.shape
    rows, _, step_count = samples.shape
    peers = sens_size - 1
    plan = Plan(bins_dev, slots, sites)
    group, chunks, m, pad = plan.group, plan.chunks, plan.m, plan.pad
    forward, inverse = make_tables(freq_size, plan, step_count)
    tiles = response_tiles.transpose(0, 3, 1, 2)
    lane_tiles = -(-slots // LANES)
    count = len(plan.pieces)
    wide = -(-step_count // LANES) * LANES
    vmem = pl.BlockSpec(memory_space=pltpu.VMEM)
    anywhere = pl.BlockSpec(memory_space=pl.ANY)
    operands = (
        tiles, samples, jnp.asarray(forward, jnp.bfloat16), jnp.asarray(inverse, jnp.bfloat16),
        slot_sensor, sensor_noise, advance_offset,
    )
    outlook, spread = pl.pallas_call(
        functools.partial(kernel, freq_size, sens_size, plan),
        out_shape=(
            jax.ShapeDtypeStruct((sites, rows, step_count), jnp.bfloat16),
            jax.ShapeDtypeStruct((1, sites), jnp.float32),
        ),
        in_specs=[anywhere] * 7,
        out_specs=(vmem, vmem),
        scratch_shapes=[
            pltpu.VMEM(tiles.shape, jnp.bfloat16),
            pltpu.VMEM(samples.shape, jnp.bfloat16),
            pltpu.VMEM(forward.shape, jnp.bfloat16),
            pltpu.VMEM(inverse.shape, jnp.bfloat16),
            pltpu.SMEM(slot_sensor.shape, jnp.int32),
            pltpu.SMEM(sensor_noise.shape, jnp.float32),
            pltpu.SMEM(advance_offset.shape, jnp.int32),
            pltpu.SemaphoreType.DMA((6,)),
            pltpu.SemaphoreType.DMA((count,)),
            pltpu.VMEM((2, slots, LANES), jnp.float32),
            pltpu.VMEM((plan.kept, LANES), jnp.float32),
            pltpu.VMEM((slots, wide), jnp.bfloat16),
            pltpu.VMEM((freq_size * 2 * pad, LANES), jnp.float32),
            pltpu.VMEM((freq_size * 2 * pad, LANES), jnp.float32),
            pltpu.VMEM((freq_size * 2 * pad, LANES), jnp.float32),
            pltpu.VMEM((2, freq_size, plan.held_rows, LANES), jnp.bfloat16),
            pltpu.VMEM((lane_tiles, freq_size * chunks * group * 2 * rows, LANES), jnp.float32),
            pltpu.VMEM((freq_size * 2 * m * rows, LANES), jnp.float32),
            pltpu.VMEM((freq_size, 2, m, rows, LANES), jnp.bfloat16),
            pltpu.VMEM((peers, freq_size, 2, m, rows, LANES), jnp.bfloat16),
            pltpu.VMEM((2, pad * rows, LANES), jnp.float32),
            pltpu.VMEM((4 * group * pad, rows * SEAT), jnp.bfloat16),
            pltpu.VMEM((rows * SEAT, step_count), jnp.float32),
            pltpu.VMEM((wide // LANES, sites * rows, LANES), jnp.float32),
            pltpu.VMEM((8, LANES), jnp.float32),
            pltpu.VMEM((8, LANES), jnp.float32),
            pltpu.VMEM((peers, 8, LANES), jnp.float32),
            pltpu.SemaphoreType.DMA((2,)),
            pltpu.SemaphoreType.DMA((count, freq_size - 1)),
            pltpu.SemaphoreType.DMA((1,)),
            pltpu.SemaphoreType.DMA((freq_size + 1,)),
            pltpu.SemaphoreType.DMA((1,)),
            pltpu.SemaphoreType.DMA((1,)),
        ],
        compiler_params=pltpu.CompilerParams(
            collective_id=0, has_side_effects=True, vmem_limit_bytes=50 * 1024 * 1024
        ),
    )(*(pltpu.with_memory_space_constraint(array, pltpu.HBM) for array in operands))
    outlook, spread = pl.pallas_call(
        hand_out,
        out_shape=(
            jax.ShapeDtypeStruct(outlook.shape, outlook.dtype),
            jax.ShapeDtypeStruct(spread.shape, spread.dtype),
        ),
        in_specs=[anywhere] * 2,
        out_specs=(anywhere, anywhere),
        scratch_shapes=[pltpu.SemaphoreType.DMA((2,))],
        compiler_params=pltpu.CompilerParams(vmem_limit_bytes=1024 * 1024),
    )(outlook, spread)
    return (outlook.transpose(1, 0, 2), spread.reshape(sites))


def solution(mesh):
    placed = (P("freq", "sens", None), P("freq", None, "sens", None), P("sens"), P(), P())
    return jax.shard_map(
        functools.partial(on_device, mesh.shape["freq"], mesh.shape["sens"]),
        mesh=mesh,
        in_specs=placed,
        out_specs=(P("freq", None, None), P()),
        check_vma=False,
    )
```
